32 devices in a mesh: dp: 1 (over z), tp: 32 (over x, y, core).
Axes of the slice: x: 4, y: 4, z: 1, core: 2. Of those that a mesh axis runs over, the one named last changes fastest.
The devices are a block of a 4x4x8 slice.
Arguments:
- x: bfloat16 [2048, 5120], P('dp')
- dy: bfloat16 [2048, 5120], P('dp')
- gate: bfloat16 [2048, 12288], P('dp', 'tp')
- up: bfloat16 [2048, 12288], P('dp', 'tp')
- w_gate: bfloat16 [5120, 12288], P(None, 'tp')
- w_up: bfloat16 [5120, 12288], P(None, 'tp')
- w_down: bfloat16 [12288, 5120], P('tp')
Outputs:
- output 1: bfloat16 [2048, 5120], P('dp')
- output 2: bfloat16 [5120, 12288], P('dp', 'tp')
- output 3: bfloat16 [5120, 12288], P('dp', 'tp')
- output 4: bfloat16 [12288, 5120], P(('dp', 'tp'))
All inputs are finite; a program needn't handle non-finite values.
Results may differ from the reference program's by a relative error of at most 0.012.
Values are sent between devices in bfloat16 or wider.
A program may use at most 768 MiB of HBM per device.

```python
import jax
import jax.numpy as jnp

ROWS = 2048
D = 5120
FF = 12288


def act(gate, up):
    return jax.nn.silu(gate) * up


def setup_inputs(seed: int = 0, part: int = 0) -> dict:
    kx, ky, ka, kb, kg, ku, kd = jax.random.split(jax.random.key(seed), 7)
    kx, ky, ka, kb = (jax.random.fold_in(k, part) for k in (kx, ky, ka, kb))
    drawn = {
        "x": jax.random.normal(kx, (ROWS, D), jnp.float32),
        "dy": jax.random.normal(ky, (ROWS, D), jnp.float32),
        "gate": jax.random.normal(ka, (ROWS, FF), jnp.float32),
        "up": jax.random.normal(kb, (ROWS, FF), jnp.float32),
        "w_gate": jax.random.normal(kg, (D, FF), jnp.float32) * D**-0.5,
        "w_up": jax.random.normal(ku, (D, FF), jnp.float32) * D**-0.5,
        "w_down": jax.random.normal(kd, (FF, D), jnp.float32) * FF**-0.5,
    }
    return {k: v.astype(jnp.bfloat16) for k, v in drawn.items()}


def reference(x, dy, gate, up, w_gate, w_up, w_down):
    hidden, back = jax.vjp(act, gate.astype(jnp.float32), up.astype(jnp.float32))
    d_hidden = jnp.dot(dy, w_down.T, preferred_element_type=jnp.float32)
    d_gate, d_up = (g.astype(jnp.bfloat16) for g in back(d_hidden))
    dx = jnp.dot(d_gate, w_gate.T, preferred_element_type=jnp.float32) + jnp.dot(d_up, w_up.T, preferred_element_type=jnp.float32)
    dw_gate = jnp.dot(x.T, d_gate, preferred_element_type=jnp.float32)
    dw_up = jnp.dot(x.T, d_up, preferred_element_type=jnp.float32)
    dw_down = jnp.dot(hidden.astype(jnp.bfloat16).T, dy, preferred_element_type=jnp.float32)
    return tuple(g.astype(jnp.bfloat16) for g in (dx, dw_gate, dw_up, dw_down))
```

```python
import functools
import math

import jax
import jax.numpy as jnp
from jax import lax
from jax.experimental import pallas as pl
from jax.experimental.pallas import tpu as pltpu
from jax.sharding import PartitionSpec as P

MESH = pl.DeviceIdType.MESH
HALF = 256
SLOTS = 3
COLS = 256
F32, BF16 = jnp.float32, jnp.bfloat16
NT = (((1,), (1,)), ((), ()))
TN = (((0,), (0,)), ((), ()))
NN = (((1,), (0,)), ((), ()))


def dot(a, b, dims):
    return lax.dot_general(a, b, dims, preferred_element_type=F32)


def kernel(
    n, x, dy, gate, up, w_gate, w_up, w_down,
    dx, dw_gate, dw_up, dw_down,
    wd, wgu, dgu, hid, sums, outbox, dy_rows, g_rows, u_rows, x_cols, dy_cols, st_gu, st_d,
    ring_send, ring_recv, pair_send, pair_recv, credit, w_sem, row_sem, col_sem, out_sem,
):
    rows, width = x.shape
    ff = gate.shape[1]
    chunks = rows // (2 * HALF)
    block = width // n
    sub = HALF // n
    hr, hc = HALF // 2, block // 2
    units = width // COLS

    me = lax.axis_index("tp")
    c = lax.rem(me, 2)
    chip = me // 2
    px, py = chip // n, lax.rem(chip, n)
    p1 = px * (1 - c) + py * c
    p2 = py * (1 - c) + px * c

    def device(ax, ay, core):
        return (lax.rem(ax, n) * n + lax.rem(ay, n)) * 2 + core

    sx, sy = 1 - c, c
    right1, left1 = device(px + sx, py + sy, c), device(px + n - sx, py + n - sy, c)
    right2, left2 = device(px + sy, py + sx, c), device(px + n - sy, py + n - sx, c)
    partner = device(px, py, 1 - c)
    q1 = px * c + py * (1 - c)

    def mod(v):
        return lax.rem(v + n, n)

    def own(k):
        return pl.multiple_of((2 * k + c) * HALF, HALF)

    def other(k):
        return pl.multiple_of((2 * k + 1 - c) * HALF, HALF)

    def cols(b):
        return pl.multiple_of(b * block, 128)

    def remote(src, dst, ssem, rsem, to):
        return pltpu.make_async_remote_copy(
            src_ref=src, dst_ref=dst, send_sem=ssem, recv_sem=rsem, device_id={"tp": to}, device_id_type=MESH
        )

    def rs1_src(k, b, h):
        return sums.at[lax.rem(k, SLOTS), b, pl.ds(h * hr, hr), :]

    def rs1_land(k, area, h):
        return dx.at[pl.ds(other(k) + h * hr, hr), pl.ds(area * block, block)]

    def rs2_src(k, s, h):
        return sums.at[lax.rem(k, SLOTS), p1, pl.ds(pl.multiple_of(s * sub, sub), sub), pl.ds(h * hc, hc)]

    def rs2_land(k, area, h):
        return dx.at[pl.ds(other(k) + area * sub, sub), pl.ds(3 * block + h * hc, hc)]

    def ag2_at(k, s, h):
        return dx.at[pl.ds(own(k) + pl.multiple_of(s * sub, sub), sub), pl.ds(cols(p1) + h * hc, hc)]

    def ag1_at(k, b, h):
        return dx.at[pl.ds(own(k) + h * hr, hr), pl.ds(cols(b), block)]

    land = {0: (0, 0), 1: (0, 1), 2: (1, 1), 3: (2, 0), 4: (1, 0), 5: (2, 1)}

    def reduce_pair(src, dst, p, i):
        which = {0: (2, 0), 1: (2, 1), 2: (n - 1, 1), 3: (1, 0), 4: (n - 1, 0), 5: (1, 1)}[i]
        return src(mod(p + which[0]), which[1]), dst(*land[i])

    def gather_at(at, p, i, arriving):
        off, h = {0: (0, 0), 1: (0, 1), 2: (0, 1), 3: (0, 0), 4: (1, 0), 5: (n - 1, 1)}[i]
        step = (1 if i % 2 == 0 else n - 1) if arriving else 0
        return at(mod(p + off + step), h)

    def ring(phase, k, i, arriving=False):
        left, right = (left1, right1) if phase in (0, 3) else (left2, right2)
        if phase == 0:
            src, dst = reduce_pair(functools.partial(rs1_src, k), functools.partial(rs1_land, k), p1, i)
        elif phase == 1:
            src, dst = reduce_pair(functools.partial(rs2_src, k), functools.partial(rs2_land, k), p2, i)
        elif phase == 2:
            src = dst = gather_at(functools.partial(ag2_at, k), p2, i, arriving)
        else:
            src = dst = gather_at(functools.partial(ag1_at, k), p1, i, arriving)
        to = left if i % 2 == 0 else right
        return remote(src, dst, ring_send.at[k, phase, i], ring_recv.at[k, phase, i], to)

    def send(phase, k, *which):
        for i in which:
            ring(phase, k, i).start()

    def arrive(phase, k, *which):
        for i in which:
            ring(phase, k, i, arriving=True).wait_recv()

    def reduced(k):
        for phase in (0, 1):
            for i in range(6):
                ring(phase, k, i).wait_send()

    def swap(k, o):
        b = lax.rem(q1 + 2 + o, n)
        return remote(
            outbox.at[o], dx.at[pl.ds(other(k), HALF), pl.ds(cols(b), block)],
            pair_send.at[k, o], pair_recv.at[k, o], partner,
        )

    def swap_in(k, o):
        b = lax.rem(p1 + 2 + o, n)
        return remote(
            outbox.at[o], dx.at[pl.ds(own(k), HALF), pl.ds(cols(b), block)],
            pair_send.at[k, o], pair_recv.at[k, o], partner,
        )

    def share(k, i):
        b = mod(p1 + (0, 1, n - 1, 2)[i])
        at = dx.at[pl.ds(own(k), HALF), pl.ds(cols(b), block)]
        return remote(at, at, pair_send.at[k, 4 + i], pair_recv.at[k, 4 + i], partner)

    def share_in(k, i):
        b = mod(q1 + (0, 1, n - 1, 2)[i])
        at = dx.at[pl.ds(other(k), HALF), pl.ds(cols(b), block)]
        return remote(at, at, pair_send.at[k, 4 + i], pair_recv.at[k, 4 + i], partner)

    def row_copies(b):
        at = pl.ds(pl.multiple_of((2 * (b // 2) + lax.rem(b + 1 + c, 2)) * HALF, HALF), HALF)
        slot = lax.rem(b, 2)
        return [
            pltpu.make_async_copy(src.at[at, :], dst.at[slot], row_sem.at[slot, i])
            for i, (src, dst) in enumerate(((dy, dy_rows), (gate, g_rows), (up, u_rows)))
        ]

    def col_copies(u):
        at = pl.ds(pl.multiple_of(u * COLS, COLS), COLS)
        slot = lax.rem(u, 2)
        return [
            pltpu.make_async_copy(src.at[:, at], dst.at[slot], col_sem.at[slot, i])
            for i, (src, dst) in enumerate(((x, x_cols), (dy, dy_cols)))
        ]

    def out_copies(u):
        at = pl.ds(pl.multiple_of(u * COLS, COLS), COLS)
        slot = lax.rem(u, 2)
        return [
            pltpu.make_async_copy(st_gu.at[slot, :, pl.ds(0, ff)], dw_gate.at[at, :], out_sem.at[slot, 0]),
            pltpu.make_async_copy(st_gu.at[slot, :, pl.ds(ff, ff)], dw_up.at[at, :], out_sem.at[slot, 1]),
            pltpu.make_async_copy(st_d.at[slot], dw_down.at[:, at], out_sem.at[slot, 2]),
        ]

    load_wd = pltpu.make_async_copy(w_down, wd, w_sem.at[0])
    load_wg = pltpu.make_async_copy(w_gate, wgu.at[:, pl.ds(0, ff)], w_sem.at[1])
    load_wu = pltpu.make_async_copy(w_up, wgu.at[:, pl.ds(ff, ff)], w_sem.at[2])

    def hidden_grads(b):
        for copy in row_copies(b):
            copy.wait()
        slot = lax.rem(b, 2)
        at = pl.multiple_of((2 * (b // 2) + lax.rem(b + 1 + c, 2)) * HALF, HALF)
        d_hidden = dot(dy_rows[slot], wd[...], NT)
        g, u = g_rows[slot].astype(F32), u_rows[slot].astype(F32)
        sig = jax.nn.sigmoid(g)
        silu = g * sig
        dgu[pl.ds(at, HALF), pl.ds(0, ff)] = (d_hidden * u * (sig + silu * (1.0 - sig))).astype(BF16)
        dgu[pl.ds(at, HALF), pl.ds(ff, ff)] = (d_hidden * silu).astype(BF16)
        hid[:, pl.ds(at, HALF)] = (silu * u).T.astype(BF16)

        @pl.when(b + 2 < 2 * chunks)
        def _():
            for copy in row_copies(b + 2):
                copy.start()

    def term(at, b):
        return dot(dgu[pl.ds(at, HALF), :], wgu[pl.ds(pl.multiple_of(b * block, 128), block), :], NT)

    def partner_half(k):
        hidden_grads(2 * k)

        @pl.when(k == 0)
        def _():
            load_wg.wait()
            load_wu.wait()

        @pl.loop(0, n)
        def _(o):
            @pl.when(k > 0)
            def _():
                swap(k - 1, o).wait_send()

            outbox[o] = term(other(k), lax.rem(q1 + 2 + o, n)).astype(BF16)
            swap(k, o).start()

    def own_half(k):
        hidden_grads(2 * k + 1)
        pl.when(k >= SLOTS)(lambda: reduced(k - SLOTS))

        @pl.loop(0, n)
        def _(o):
            b = lax.rem(p1 + 2 + o, n)
            t = term(own(k), b)
            swap_in(k, o).wait_recv()
            sums[lax.rem(k, SLOTS), b] = (t + dx[pl.ds(own(k), HALF), pl.ds(cols(b), block)].astype(F32)).astype(BF16)

            @pl.when(o == 0)
            def _():
                send(0, k, 0, 1)

            @pl.when(o == 1)
            def _():
                send(0, k, 2)

            @pl.when(o == 3)
            def _():
                send(0, k, 3)

    def weight_grads(u):
        for copy in col_copies(u):
            copy.wait()
        slot = lax.rem(u, 2)

        @pl.when(u >= 2)
        def _():
            for copy in out_copies(u - 2):
                copy.wait()

        st_gu[slot] = dot(x_cols[slot], dgu[...], TN).astype(BF16)
        st_d[slot] = dot(hid[...], dy_cols[slot], NN).astype(BF16)
        for copy in out_copies(u):
            copy.start()

        @pl.when(u + 2 < units)
        def _():
            for copy in col_copies(u + 2):
                copy.start()

    def add(dst, size, *srcs):
        step = 32

        @pl.loop(0, size // step)
        def _(r):
            at = pl.multiple_of(r * step, step)
            total = srcs[0](at, step).astype(F32)
            for s in srcs[1:]:
                total = total + s(at, step).astype(F32)
            dst(at, step, total.astype(BF16))

    def add_sums(k, b, off, size, lanes, *lands):
        def mine(at, step):
            return sums[lax.rem(k, SLOTS), b, pl.ds(off + at, step), lanes]

        def put(at, step, v):
            sums[lax.rem(k, SLOTS), b, pl.ds(off + at, step), lanes] = v

        add(put, size, mine, *lands)

    def landed(row, first, wide):
        return lambda at, step: dx[pl.ds(row + at, step), pl.ds(first, wide)]

    def s1(k):
        arrive(0, k, 0)
        add_sums(k, mod(p1 + n - 1), 0, hr, slice(None), landed(other(k), 0, block))
        send(0, k, 4)
        arrive(0, k, 1)
        add_sums(k, mod(p1 + 1), hr, hr, slice(None), landed(other(k) + hr, 0, block))
        send(0, k, 5)

    def s2(k):
        arrive(0, k, 2, 3, 4, 5)
        add_sums(k, p1, 0, HALF, slice(None), landed(other(k), block, block), landed(other(k), 2 * block, block))
        send(1, k, 0, 1, 2, 3)

    def s3(k):
        base = 3 * block
        arrive(1, k, 0)
        add_sums(k, p1, pl.multiple_of(mod(p2 + n - 1) * sub, sub), sub, pl.ds(0, hc), landed(other(k), base, hc))
        send(1, k, 4)
        arrive(1, k, 1)
        add_sums(k, p1, pl.multiple_of(mod(p2 + 1) * sub, sub), sub, pl.ds(hc, hc), landed(other(k), base + hc, hc))
        send(1, k, 5)

    def s4(k):
        arrive(1, k, 2, 3, 4, 5)
        off = pl.multiple_of(p2 * sub, sub)

        def put(at, step, v):
            dx[pl.ds(own(k) + off + at, step), pl.ds(cols(p1), block)] = v

        add(
            put, sub,
            lambda at, step: sums[lax.rem(k, SLOTS), p1, pl.ds(off + at, step), :],
            landed(other(k) + sub, 3 * block, block),
            landed(other(k) + 2 * sub, 3 * block, block),
        )
        send(2, k, 0, 1, 2, 3)
        pl.semaphore_signal(credit.at[k], inc=1, device_id={"tp": partner}, device_id_type=MESH)

    def s5(k):
        arrive(2, k, 0)
        send(2, k, 4)
        arrive(2, k, 1)
        send(2, k, 5)

    def s6(k):
        arrive(2, k, 2, 3, 4, 5)
        send(3, k, 0, 1, 2, 3)
        pl.semaphore_wait(credit.at[k], 1)
        share(k, 0).start()

    def s7(k):
        arrive(3, k, 0)
        send(3, k, 4)
        arrive(3, k, 1)
        send(3, k, 5)

    def s8(k):
        arrive(3, k, 2)
        share(k, 1).start()
        arrive(3, k, 3)
        share(k, 2).start()
        arrive(3, k, 4, 5)
        share(k, 3).start()

    def s9(k):
        for i in range(n):
            share_in(k, i).wait_recv()

    def at_chunk(stage, k):
        pl.when(jnp.logical_and(k >= 0, k < chunks))(lambda: stage(k))

    def some_units(slot):
        @pl.loop(0, 4)
        def _(i):
            u = slot * 4 + i
            pl.when(u < units)(lambda: weight_grads(u))

    load_wd.start()
    for b in range(2):
        for copy in row_copies(b):
            copy.start()
    load_wg.start()
    load_wu.start()
    barrier = pltpu.get_barrier_semaphore()
    for to in (left1, right1, left2, right2, partner):
        pl.semaphore_signal(barrier, inc=1, device_id={"tp": to}, device_id_type=MESH)
    pl.semaphore_wait(barrier, 5)
    load_wd.wait()

    @pl.loop(0, chunks + 5)
    def _(j):
        late = j >= chunks
        pl.when(j < chunks)(lambda: partner_half(j))
        pl.when(late)(lambda: some_units(2 * (j - chunks)))
        at_chunk(s1, j - 1)
        at_chunk(s3, j - 2)
        at_chunk(s5, j - 3)
        at_chunk(s7, j - 4)
        at_chunk(s9, j - 5)
        pl.when(j < chunks)(lambda: own_half(j))

        @pl.when(j == 1)
        def _():
            for u in range(2):
                for copy in col_copies(u):
                    copy.start()

        pl.when(late)(lambda: some_units(2 * (j - chunks) + 1))
        at_chunk(s2, j - 1)
        at_chunk(s4, j - 2)
        at_chunk(s6, j - 3)
        at_chunk(s8, j - 4)

    @pl.loop(0, chunks)
    def _(k):
        pl.when(k >= chunks - SLOTS)(lambda: reduced(k))
        for phase in (2, 3):
            for i in range(6):
                ring(phase, k, i).wait_send()
        for i in range(n):
            share(k, i).wait_send()

    @pl.loop(0, n)
    def _(o):
        swap(chunks - 1, o).wait_send()

    for u in (units - 2, units - 1):
        for copy in out_copies(u):
            copy.wait()


def solution(mesh):
    n = math.isqrt(mesh.shape["tp"] // 2)
    if n != 4 or 2 * n * n != mesh.shape["tp"]:
        raise ValueError("unexpected group")

    def step(x, dy, gate, up, w_gate, w_up, w_down):
        rows, width = x.shape
        ff = gate.shape[1]
        chunks, block = rows // (2 * HALF), width // n
        any_space = pl.BlockSpec(memory_space=pl.ANY)
        vmem = pl.BlockSpec(memory_space=pltpu.VMEM)
        dma = pltpu.SemaphoreType.DMA
        dx, dw_gate, dw_up, dw_down = pl.pallas_call(
            functools.partial(kernel, n),
            out_shape=(
                pltpu.VMEM(x.shape, BF16),
                jax.ShapeDtypeStruct(w_gate.shape, BF16),
                jax.ShapeDtypeStruct(w_up.shape, BF16),
                jax.ShapeDtypeStruct(w_down.shape, BF16),
            ),
            in_specs=[any_space] * 7,
            out_specs=(vmem, any_space, any_space, any_space),
            scratch_shapes=[
                pltpu.VMEM((ff, width), BF16),
                pltpu.VMEM((width, 2 * ff), BF16),
                pltpu.VMEM((rows, 2 * ff), BF16),
                pltpu.VMEM((ff, rows), BF16),
                pltpu.VMEM((SLOTS, n, HALF, block), BF16),
                pltpu.VMEM((n, HALF, block), BF16),
                pltpu.VMEM((2, HALF, width), BF16),
                pltpu.VMEM((2, HALF, ff), BF16),
                pltpu.VMEM((2, HALF, ff), BF16),
                pltpu.VMEM((2, rows, COLS), BF16),
                pltpu.VMEM((2, rows, COLS), BF16),
                pltpu.VMEM((2, COLS, 2 * ff), BF16),
                pltpu.VMEM((2, ff, COLS), BF16),
                dma((chunks, 4, 6)),
                dma((chunks, 4, 6)),
                dma((chunks, 2 * n)),
                dma((chunks, 2 * n)),
                pltpu.SemaphoreType.REGULAR((chunks,)),
                dma((3,)),
                dma((2, 3)),
                dma((2, 2)),
                dma((2, 3)),
            ],
            compiler_params=pltpu.CompilerParams(
                collective_id=0, has_side_effects=True, vmem_limit_bytes=700 * 64 * 1024
            ),
        )(x, dy, gate, up, w_gate, w_up, w_down)
        return dx, dw_gate, dw_up, dw_down

    tokens, columns, by_rows = P("dp", None), P(None, "tp"), P("tp", None)
    return jax.shard_map(
        step,
        mesh=mesh,
        in_specs=(tokens, tokens, P("dp", "tp"), P("dp", "tp"), columns, columns, by_rows),
        out_specs=(tokens, P("dp", "tp"), P("dp", "tp"), P(("dp", "tp"), None)),
        check_vma=False,
    )
```

```python
import functools
import math

import jax
import jax.numpy as jnp
from jax import lax
from jax.experimental import pallas as pl
from jax.experimental.pallas import tpu as pltpu
from jax.sharding import PartitionSpec as P

MESH = pl.DeviceIdType.MESH
HALF = 256
SLOTS = 3
PERIOD = 10
TICKS = (
    (10, 20, 30, 40),
    (17, 27, 37, 45),
    (21, 31, 41, 48),
    (25, 35, 44, 51),
    (29, 39, 47, 54),
    (41, 43, 49, 57),
    (46, 50, 55, 61),
    (52, 57, 62, 66),
    (56, 62, 66, 70),
)
COLS = 256
F32, BF16 = jnp.float32, jnp.bfloat16
NT = (((1,), (1,)), ((), ()))
TN = (((0,), (0,)), ((), ()))
NN = (((1,), (0,)), ((), ()))


def dot(a, b, dims):
    return lax.dot_general(a, b, dims, preferred_element_type=F32)


def scoped(stage):
    def named(*args):
        with jax.named_scope(stage.__name__):
            return stage(*args)

    return named


def kernel(
    n, x, dy, gate, up, w_gate, w_up, w_down,
    wgu, wd, mine, theirs,
    dgu, hid, sums, outbox, dy_rows, g_rows, u_rows, x_cols, dy_cols,
    ring_send, ring_recv, pair_send, pair_recv, credit, w_sem, row_sem, col_sem,
):
    rows, width = x.shape
    ff = gate.shape[1]
    chunks = rows // (2 * HALF)
    block = width // n
    sub = HALF // n
    hr, hc = HALF // 2, block // 2
    units = width // COLS

    me = lax.axis_index("tp")
    c = lax.rem(me, 2)
    chip = me // 2
    px, py = chip // n, lax.rem(chip, n)
    p1 = px * (1 - c) + py * c
    p2 = py * (1 - c) + px * c

    def device(ax, ay, core):
        return (lax.rem(ax, n) * n + lax.rem(ay, n)) * 2 + core

    sx, sy = 1 - c, c
    right1, left1 = device(px + sx, py + sy, c), device(px + n - sx, py + n - sy, c)
    right2, left2 = device(px + sy, py + sx, c), device(px + n - sy, py + n - sx, c)
    partner = device(px, py, 1 - c)
    q1 = px * c + py * (1 - c)

    def mod(v):
        return lax.rem(v + n, n)

    def own(k):
        return pl.multiple_of((2 * k + c) * HALF, HALF)

    def other(k):
        return pl.multiple_of((2 * k + 1 - c) * HALF, HALF)

    def turn(o):
        return (2 + o) * (1 - o // 2) + (3 - o) * (o // 2)

    def kept(k):
        return pl.multiple_of(k * HALF, HALF)

    def cols(b):
        return pl.multiple_of(b * block, 128)

    def remote(src, dst, ssem, rsem, to):
        return pltpu.make_async_remote_copy(
            src_ref=src, dst_ref=dst, send_sem=ssem, recv_sem=rsem, device_id={"tp": to}, device_id_type=MESH
        )

    def rs1_src(k, b, h):
        return sums.at[lax.rem(k, SLOTS), b, pl.ds(h * hr, hr), :]

    def rs1_land(k, area, h):
        return theirs.at[pl.ds(kept(k) + h * hr, hr), pl.ds(area * block, block)]

    def rs2_src(k, s, h):
        return sums.at[lax.rem(k, SLOTS), p1, pl.ds(pl.multiple_of(s * sub, sub), sub), pl.ds(h * hc, hc)]

    def rs2_land(k, area, h):
        return theirs.at[pl.ds(kept(k) + area * sub, sub), pl.ds(3 * block + h * hc, hc)]

    def ag2_at(k, s, h):
        return mine.at[pl.ds(kept(k) + pl.multiple_of(s * sub, sub), sub), pl.ds(cols(p1) + h * hc, hc)]

    def ag1_at(k, b, h):
        return mine.at[pl.ds(kept(k) + h * hr, hr), pl.ds(cols(b), block)]

    land = {0: (0, 0), 1: (0, 1), 2: (1, 1), 3: (2, 0), 4: (1, 0), 5: (2, 1)}

    def reduce_pair(src, dst, p, i):
        which = {0: (2, 0), 1: (2, 1), 2: (n - 1, 1), 3: (1, 0), 4: (n - 1, 0), 5: (1, 1)}[i]
        return src(mod(p + which[0]), which[1]), dst(*land[i])

    def gather_at(at, p, i, arriving):
        off, h = {0: (0, 0), 1: (0, 1), 2: (0, 1), 3: (0, 0), 4: (1, 0), 5: (n - 1, 1)}[i]
        step = (1 if i % 2 == 0 else n - 1) if arriving else 0
        return at(mod(p + off + step), h)

    def ring(phase, k, i, arriving=False):
        left, right = (left1, right1) if phase in (0, 3) else (left2, right2)
        if phase == 0:
            src, dst = reduce_pair(functools.partial(rs1_src, k), functools.partial(rs1_land, k), p1, i)
        elif phase == 1:
            src, dst = reduce_pair(functools.partial(rs2_src, k), functools.partial(rs2_land, k), p2, i)
        elif phase == 2:
            src = dst = gather_at(functools.partial(ag2_at, k), p2, i, arriving)
        else:
            src = dst = gather_at(functools.partial(ag1_at, k), p1, i, arriving)
        to = left if i % 2 == 0 else right
        return remote(src, dst, ring_send.at[k, phase, i], ring_recv.at[k, phase, i], to)

    def send(phase, k, *which):
        for i in which:
            ring(phase, k, i).start()

    def arrive(phase, k, *which):
        for i in which:
            ring(phase, k, i, arriving=True).wait_recv()

    def reduced(k):
        for phase in (0, 1):
            for i in range(6):
                ring(phase, k, i).wait_send()

    def swap(k, o):
        b = lax.rem(q1 + turn(o), n)
        return remote(
            outbox.at[o], mine.at[pl.ds(kept(k), HALF), pl.ds(cols(b), block)],
            pair_send.at[k, o], pair_recv.at[k, o], partner,
        )

    def swap_in(k, o):
        b = lax.rem(p1 + turn(o), n)
        return remote(
            outbox.at[o], mine.at[pl.ds(kept(k), HALF), pl.ds(cols(b), block)],
            pair_send.at[k, o], pair_recv.at[k, o], partner,
        )

    def share(k, i):
        b = mod(p1 + (0, 1, n - 1, 2)[i])
        at = pl.ds(kept(k), HALF), pl.ds(cols(b), block)
        return remote(mine.at[at], theirs.at[at], pair_send.at[k, 4 + i], pair_recv.at[k, 4 + i], partner)

    def share_in(k, i):
        b = mod(q1 + (0, 1, n - 1, 2)[i])
        at = pl.ds(kept(k), HALF), pl.ds(cols(b), block)
        return remote(mine.at[at], theirs.at[at], pair_send.at[k, 4 + i], pair_recv.at[k, 4 + i], partner)

    def row_copies(b):
        at = pl.ds(pl.multiple_of((2 * (b // 2) + lax.rem(b + 1 + c, 2)) * HALF, HALF), HALF)
        slot = lax.rem(b, 2)
        return [
            pltpu.make_async_copy(src.at[at, :], dst.at[slot], row_sem.at[slot, i])
            for i, (src, dst) in enumerate(((dy, dy_rows), (gate, g_rows), (up, u_rows)))
        ]

    def col_copies(u):
        at = pl.ds(pl.multiple_of(u * COLS, COLS), COLS)
        slot = lax.rem(u, 2)
        return [
            pltpu.make_async_copy(src.at[:, at], dst.at[slot], col_sem.at[slot, i])
            for i, (src, dst) in enumerate(((x, x_cols), (dy, dy_cols)))
        ]

    load_wd = pltpu.make_async_copy(w_down, wd, w_sem.at[0])
    def load_w(i):
        at = pl.ds(pl.multiple_of(lax.rem(q1 + turn(i), n) * block, 128), block)
        return [
            pltpu.make_async_copy(w_gate.at[at, :], wgu.at[at, pl.ds(0, ff)], w_sem.at[2 * i + 1]),
            pltpu.make_async_copy(w_up.at[at, :], wgu.at[at, pl.ds(ff, ff)], w_sem.at[2 * i + 2]),
        ]

    @scoped
    def hidden_grads(b):
        for copy in row_copies(b):
            copy.wait()
        slot = lax.rem(b, 2)
        at = pl.multiple_of((2 * (b // 2) + lax.rem(b + 1 + c, 2)) * HALF, HALF)
        d_hidden = dot(dy_rows[slot], wd[...], NT)
        g, u = g_rows[slot].astype(F32), u_rows[slot].astype(F32)
        sig = jax.nn.sigmoid(g)
        silu = g * sig
        dgu[pl.ds(at, HALF), pl.ds(0, ff)] = (d_hidden * u * (sig + silu * (1.0 - sig))).astype(BF16)
        dgu[pl.ds(at, HALF), pl.ds(ff, ff)] = (d_hidden * silu).astype(BF16)
        hid[:, pl.ds(at, HALF)] = (silu * u).T.astype(BF16)

        @pl.when(b + 2 < 2 * chunks)
        def _():
            for copy in row_copies(b + 2):
                copy.start()

    def term(at, b):
        return dot(dgu[pl.ds(at, HALF), :], wgu[pl.ds(pl.multiple_of(b * block, 128), block), :], NT)

    @scoped
    def partner_block(k, o):
        @pl.when(jnp.logical_and(k == 0, o == 0))
        def _():
            for copy in load_w(0):
                copy.wait()

        @pl.when(jnp.logical_and(k == 0, o == 1))
        def _():
            for i in range(1, n):
                for copy in load_w(i):
                    copy.wait()

        pl.when(k > 0)(lambda: swap(k - 1, o).wait_send())
        outbox[o] = term(other(k), lax.rem(q1 + turn(o), n)).astype(BF16)
        swap(k, o).start()

    @scoped
    def own_block(k, o):
        pl.when(jnp.logical_and(k >= SLOTS, o == 0))(lambda: reduced(k - SLOTS))
        b = lax.rem(p1 + turn(o), n)
        t = term(own(k), b)
        swap_in(k, o).wait_recv()
        sums[lax.rem(k, SLOTS), b] = (t + mine[pl.ds(kept(k), HALF), pl.ds(cols(b), block)].astype(F32)).astype(BF16)
        pl.when(o == 0)(lambda: send(0, k, 0, 1))
        pl.when(o == 1)(lambda: send(0, k, 2))
        pl.when(o == 2)(lambda: send(0, k, 3))

    @scoped
    def weight_grads(u):
        for copy in col_copies(u):
            copy.wait()
        slot = lax.rem(u, 2)

        at = pl.ds(pl.multiple_of(u * COLS, COLS), COLS)
        wgu[at, :] = dot(x_cols[slot], dgu[...], TN).astype(BF16)
        wd[:, at] = dot(hid[...], dy_cols[slot], NN).astype(BF16)

        @pl.when(u + 2 < units)
        def _():
            for copy in col_copies(u + 2):
                copy.start()

    def add(dst, size, *srcs):
        step = 32

        @pl.loop(0, size // step)
        def _(r):
            at = pl.multiple_of(r * step, step)
            total = srcs[0](at, step).astype(F32)
            for s in srcs[1:]:
                total = total + s(at, step).astype(F32)
            dst(at, step, total.astype(BF16))

    def add_sums(k, b, off, size, lanes, *lands):
        def mine(at, step):
            return sums[lax.rem(k, SLOTS), b, pl.ds(off + at, step), lanes]

        def put(at, step, v):
            sums[lax.rem(k, SLOTS), b, pl.ds(off + at, step), lanes] = v

        add(put, size, mine, *lands)

    def landed(row, first, wide):
        return lambda at, step: theirs[pl.ds(row + at, step), pl.ds(first, wide)]

    @scoped
    def s1(k):
        arrive(0, k, 0)
        add_sums(k, mod(p1 + n - 1), 0, hr, slice(None), landed(kept(k), 0, block))
        send(0, k, 4)
        arrive(0, k, 1)
        add_sums(k, mod(p1 + 1), hr, hr, slice(None), landed(kept(k) + hr, 0, block))
        send(0, k, 5)

    @scoped
    def s2(k):
        arrive(0, k, 2, 3, 4, 5)
        add_sums(k, p1, 0, HALF, slice(None), landed(kept(k), block, block), landed(kept(k), 2 * block, block))
        send(1, k, 0, 1, 2, 3)

    @scoped
    def s3(k):
        base = 3 * block
        arrive(1, k, 0)
        add_sums(k, p1, pl.multiple_of(mod(p2 + n - 1) * sub, sub), sub, pl.ds(0, hc), landed(kept(k), base, hc))
        send(1, k, 4)
        arrive(1, k, 1)
        add_sums(k, p1, pl.multiple_of(mod(p2 + 1) * sub, sub), sub, pl.ds(hc, hc), landed(kept(k), base + hc, hc))
        send(1, k, 5)

    @scoped
    def s4(k):
        arrive(1, k, 2, 3, 4, 5)
        off = pl.multiple_of(p2 * sub, sub)

        def put(at, step, v):
            mine[pl.ds(kept(k) + off + at, step), pl.ds(cols(p1), block)] = v

        add(
            put, sub,
            lambda at, step: sums[lax.rem(k, SLOTS), p1, pl.ds(off + at, step), :],
            landed(kept(k) + sub, 3 * block, block),
            landed(kept(k) + 2 * sub, 3 * block, block),
        )
        send(2, k, 0, 1, 2, 3)
        pl.semaphore_signal(credit.at[k], inc=1, device_id={"tp": partner}, device_id_type=MESH)

    @scoped
    def s5(k):
        arrive(2, k, 0)
        send(2, k, 4)
        arrive(2, k, 1)
        send(2, k, 5)

    @scoped
    def s6(k):
        arrive(2, k, 2, 3, 4, 5)
        send(3, k, 0, 1, 2, 3)
        pl.semaphore_wait(credit.at[k], 1)
        share(k, 0).start()

    @scoped
    def s7(k):
        arrive(3, k, 0)
        send(3, k, 4)
        arrive(3, k, 1)
        send(3, k, 5)

    @scoped
    def s8(k):
        arrive(3, k, 2)
        share(k, 1).start()
        arrive(3, k, 3)
        share(k, 2).start()
        arrive(3, k, 4, 5)
        share(k, 3).start()

    @scoped
    def s9(k):
        for i in range(n):
            share_in(k, i).wait_recv()

    def matmuls(t):
        k, r = t // PERIOD, lax.rem(t, PERIOD)
        odd = lax.rem(r, 2) == 1
        last = r == PERIOD - 1

        pl.when(jnp.logical_or(r == 0, r == 2))(lambda: hidden_grads(2 * k + r // 2))
        pl.when(jnp.logical_and(odd, jnp.logical_not(last)))(lambda: partner_block(k, r // 2))
        pl.when(jnp.logical_or(last, jnp.logical_and(jnp.logical_not(odd), r >= 4)))(
            lambda: own_block(k, (r - 4 + r // (PERIOD - 1)) // 2)
        )

    stages = (s1, s2, s3, s4, s5, s6, s7, s8, s9)
    work = chunks * PERIOD

    load_wd.start()
    for copy in row_copies(0):
        copy.start()
    barrier = pltpu.get_barrier_semaphore()
    for to in (left1, right1, left2, right2, partner):
        pl.semaphore_signal(barrier, inc=1, device_id={"tp": to}, device_id_type=MESH)
    for copy in load_w(0) + row_copies(1) + load_w(1) + load_w(2) + load_w(3):
        copy.start()
    with jax.named_scope("meet"):
        pl.semaphore_wait(barrier, 5)
    with jax.named_scope("load"):
        load_wd.wait()

    @pl.loop(0, TICKS[-1][-1] + 1)
    def _(t):
        pl.when(t < work)(lambda: matmuls(t))

        @pl.when(t == PERIOD)
        def _():
            for u in range(2):
                for copy in col_copies(u):
                    copy.start()

        pl.when(jnp.logical_and(t >= work, t < work + units))(lambda: weight_grads(t - work))
        for stage, ticks in zip(stages, TICKS):
            now, k = t == ticks[0], 0
            for tick in ticks[1:]:
                now = jnp.logical_or(now, t == tick)
                k = k + (t >= tick).astype(jnp.int32)
            pl.when(now)(functools.partial(stage, k))

    @pl.loop(0, chunks)
    def _(k):
        pl.when(k >= chunks - SLOTS)(lambda: reduced(k))
        for phase in (2, 3):
            for i in range(6):
                ring(phase, k, i).wait_send()
        for i in range(n):
            share(k, i).wait_send()

    @pl.loop(0, n)
    def _(o):
        swap(chunks - 1, o).wait_send()


def store(dw_gu, dw_d, mine, theirs, dx, dw_gate, dw_up, dw_down, sem):
    c = lax.rem(lax.axis_index("tp"), 2)
    ff = dw_gate.shape[1]
    pairs = [(dw_gu.at[:, pl.ds(0, ff)], dw_gate), (dw_gu.at[:, pl.ds(ff, ff)], dw_up), (dw_d, dw_down)]
    for k in range(mine.shape[0] // HALF):
        for half, core in ((mine, c), (theirs, 1 - c)):
            at = pl.ds(pl.multiple_of((2 * k + core) * HALF, HALF), HALF)
            pairs.append((half.at[pl.ds(k * HALF, HALF), :], dx.at[at, :]))
    copies = [pltpu.make_async_copy(src, dst, sem.at[i]) for i, (src, dst) in enumerate(pairs)]
    for copy in copies:
        copy.start()
    for copy in copies:
        copy.wait()


def solution(mesh):
    n = math.isqrt(mesh.shape["tp"] // 2)
    if n != 4 or 2 * n * n != mesh.shape["tp"]:
        raise ValueError("unexpected group")

    def step(x, dy, gate, up, w_gate, w_up, w_down):
        rows, width = x.shape
        ff = gate.shape[1]
        chunks, block = rows // (2 * HALF), width // n
        any_space = pl.BlockSpec(memory_space=pl.ANY)
        vmem = pl.BlockSpec(memory_space=pltpu.VMEM)
        dma = pltpu.SemaphoreType.DMA
        kept = pl.pallas_call(
            functools.partial(kernel, n),
            out_shape=(
                pltpu.VMEM((width, 2 * ff), BF16),
                pltpu.VMEM((ff, width), BF16),
                pltpu.VMEM((rows // 2, width), BF16),
                pltpu.VMEM((rows // 2, width), BF16),
            ),
            in_specs=[any_space] * 7,
            out_specs=[vmem] * 4,
            scratch_shapes=[
                pltpu.VMEM((rows, 2 * ff), BF16),
                pltpu.VMEM((ff, rows), BF16),
                pltpu.VMEM((SLOTS, n, HALF, block), BF16),
                pltpu.VMEM((n, HALF, block), BF16),
                pltpu.VMEM((2, HALF, width), BF16),
                pltpu.VMEM((2, HALF, ff), BF16),
                pltpu.VMEM((2, HALF, ff), BF16),
                pltpu.VMEM((2, rows, COLS), BF16),
                pltpu.VMEM((2, rows, COLS), BF16),
                dma((chunks, 4, 6)),
                dma((chunks, 4, 6)),
                dma((chunks, 2 * n)),
                dma((chunks, 2 * n)),
                pltpu.SemaphoreType.REGULAR((chunks,)),
                dma((1 + 2 * n,)),
                dma((2, 3)),
                dma((2, 2)),
            ],
            compiler_params=pltpu.CompilerParams(
                collective_id=0, has_side_effects=True, vmem_limit_bytes=31 * 1024 * 1024
            ),
        )(x, dy, gate, up, w_gate, w_up, w_down)
        return pl.pallas_call(
            store,
            out_shape=[jax.ShapeDtypeStruct(a.shape, BF16) for a in (x, w_gate, w_up, w_down)],
            in_specs=[vmem] * 4,
            out_specs=[any_space] * 4,
            scratch_shapes=[dma((3 + rows // HALF,))],
            compiler_params=pltpu.CompilerParams(vmem_limit_bytes=1024 * 1024),
        )(*kept)

    tokens, columns, by_rows = P("dp", None), P(None, "tp"), P("tp", None)
    return jax.shard_map(
        step,
        mesh=mesh,
        in_specs=(tokens, tokens, P("dp", "tp"), P("dp", "tp"), columns, columns, by_rows),
        out_specs=(tokens, P("dp", "tp"), P("dp", "tp"), P(("dp", "tp"), None)),
        check_vma=False,
    )
```

```python
import functools
import math

import jax
import jax.numpy as jnp
from jax import lax
from jax.experimental import pallas as pl
from jax.experimental.pallas import tpu as pltpu
from jax.sharding import PartitionSpec as P

MESH = pl.DeviceIdType.MESH
HALF = 256
SLOTS = 3
PERIOD = 10
TICKS = (
    (10, 20, 30, 40),
    (17, 27, 37, 45),
    (21, 31, 41, 48),
    (25, 35, 44, 51),
    (29, 39, 47, 54),
    (41, 45, 52, 57),
    (48, 54, 60, 64),
    (54, 60, 65, 70),
    (58, 64, 70, 75),
)
PIECES = 4
COLS = 256
F32, BF16 = jnp.float32, jnp.bfloat16
NT = (((1,), (1,)), ((), ()))
TN = (((0,), (0,)), ((), ()))
NN = (((1,), (0,)), ((), ()))


def dot(a, b, dims):
    return lax.dot_general(a, b, dims, preferred_element_type=F32)


def scoped(stage):
    def named(*args):
        with jax.named_scope(stage.__name__):
            return stage(*args)

    return named


def kernel(
    n, x, dy, gate, up, w_gate, w_up, w_down,
    wgu, wd, mine, theirs,
    dgu, hid, sums, outbox, dy_rows, g_rows, u_rows, x_cols, dy_cols,
    ring_send, ring_recv, pair_send, pair_recv, credit, w_sem, first_sem, row_sem, col_sem,
):
    rows, width = x.shape
    ff = gate.shape[1]
    chunks = rows // (2 * HALF)
    block = width // n
    sub = HALF // n
    hr, hc = HALF // 2, block // 2
    units = width // COLS

    me = lax.axis_index("tp")
    c = lax.rem(me, 2)
    chip = me // 2
    px, py = chip // n, lax.rem(chip, n)
    p1 = px * (1 - c) + py * c
    p2 = py * (1 - c) + px * c

    def device(ax, ay, core):
        return (lax.rem(ax, n) * n + lax.rem(ay, n)) * 2 + core

    sx, sy = 1 - c, c
    right1, left1 = device(px + sx, py + sy, c), device(px + n - sx, py + n - sy, c)
    right2, left2 = device(px + sy, py + sx, c), device(px + n - sy, py + n - sx, c)
    partner = device(px, py, 1 - c)
    q1 = px * c + py * (1 - c)

    def mod(v):
        return lax.rem(v + n, n)

    def own(k):
        return pl.multiple_of((2 * k + c) * HALF, HALF)

    def other(k):
        return pl.multiple_of((2 * k + 1 - c) * HALF, HALF)

    def turn(o):
        return (2 + o) * (1 - o // 2) + (3 - o) * (o // 2)

    def kept(k):
        return pl.multiple_of(k * HALF, HALF)

    def cols(b):
        return pl.multiple_of(b * block, 128)

    def remote(src, dst, ssem, rsem, to):
        return pltpu.make_async_remote_copy(
            src_ref=src, dst_ref=dst, send_sem=ssem, recv_sem=rsem, device_id={"tp": to}, device_id_type=MESH
        )

    def rs1_src(k, b, h):
        return sums.at[lax.rem(k, SLOTS), b, pl.ds(h * hr, hr), :]

    def rs1_land(k, area, h):
        return theirs.at[pl.ds(kept(k) + h * hr, hr), pl.ds(area * block, block)]

    def rs2_src(k, s, h):
        return sums.at[lax.rem(k, SLOTS), p1, pl.ds(pl.multiple_of(s * sub, sub), sub), pl.ds(h * hc, hc)]

    def rs2_land(k, area, h):
        return theirs.at[pl.ds(kept(k) + area * sub, sub), pl.ds(3 * block + h * hc, hc)]

    def ag2_at(k, s, h):
        return mine.at[pl.ds(kept(k) + pl.multiple_of(s * sub, sub), sub), pl.ds(cols(p1) + h * hc, hc)]

    def ag1_at(k, b, h):
        return mine.at[pl.ds(kept(k) + h * hr, hr), pl.ds(cols(b), block)]

    land = {0: (0, 0), 1: (0, 1), 2: (1, 1), 3: (2, 0), 4: (1, 0), 5: (2, 1)}

    def reduce_pair(src, dst, p, i):
        which = {0: (2, 0), 1: (2, 1), 2: (n - 1, 1), 3: (1, 0), 4: (n - 1, 0), 5: (1, 1)}[i]
        return src(mod(p + which[0]), which[1]), dst(*land[i])

    def gather_at(at, p, i, arriving):
        off, h = {0: (0, 0), 1: (0, 1), 2: (0, 1), 3: (0, 0), 4: (1, 0), 5: (n - 1, 1)}[i]
        step = (1 if i % 2 == 0 else n - 1) if arriving else 0
        return at(mod(p + off + step), h)

    def ring(phase, k, i, arriving=False):
        left, right = (left1, right1) if phase in (0, 3) else (left2, right2)
        if phase == 0:
            src, dst = reduce_pair(functools.partial(rs1_src, k), functools.partial(rs1_land, k), p1, i)
        elif phase == 1:
            src, dst = reduce_pair(functools.partial(rs2_src, k), functools.partial(rs2_land, k), p2, i)
        elif phase == 2:
            src = dst = gather_at(functools.partial(ag2_at, k), p2, i, arriving)
        else:
            src = dst = gather_at(functools.partial(ag1_at, k), p1, i, arriving)
        to = left if i % 2 == 0 else right
        return remote(src, dst, ring_send.at[k, phase, i], ring_recv.at[k, phase, i], to)

    def send(phase, k, *which):
        for i in which:
            ring(phase, k, i).start()

    def arrive(phase, k, *which):
        for i in which:
            ring(phase, k, i, arriving=True).wait_recv()

    def reduced(k):
        for phase in (0, 1):
            for i in range(6):
                ring(phase, k, i).wait_send()

    def swap(k, o):
        b = lax.rem(q1 + turn(o), n)
        return remote(
            outbox.at[o], mine.at[pl.ds(kept(k), HALF), pl.ds(cols(b), block)],
            pair_send.at[k, o], pair_recv.at[k, o], partner,
        )

    def swap_in(k, o):
        b = lax.rem(p1 + turn(o), n)
        return remote(
            outbox.at[o], mine.at[pl.ds(kept(k), HALF), pl.ds(cols(b), block)],
            pair_send.at[k, o], pair_recv.at[k, o], partner,
        )

    def shared(k, i, place):
        b = mod(place + (0, 1, n - 1, 2, 2)[i])
        first, size = ((0, HALF), (0, HALF), (0, HALF), (0, hr), (hr, hr))[i]
        return pl.ds(kept(k) + first, size), pl.ds(cols(b), block)

    def share(k, i):
        at = shared(k, i, p1)
        return remote(mine.at[at], theirs.at[at], pair_send.at[k, 4 + i], pair_recv.at[k, 4 + i], partner)

    def share_in(k, i):
        at = shared(k, i, q1)
        return remote(mine.at[at], theirs.at[at], pair_send.at[k, 4 + i], pair_recv.at[k, 4 + i], partner)

    def rows_of(b):
        return pl.multiple_of((2 * (b // 2) + lax.rem(b + 1 + c, 2)) * HALF, HALF)

    def row_copies(b, first=0):
        at = pl.ds(rows_of(b), HALF)
        slot = lax.rem(b, 2)
        return [
            pltpu.make_async_copy(src.at[at, :], dst.at[slot], row_sem.at[slot, i])
            for i, (src, dst) in enumerate(((dy, dy_rows), (gate, g_rows), (up, u_rows)))
            if i >= first
        ]

    def col_copies(u):
        at = pl.ds(pl.multiple_of(u * COLS, COLS), COLS)
        slot = lax.rem(u, 2)
        return [
            pltpu.make_async_copy(src.at[:, at], dst.at[slot], col_sem.at[slot, i])
            for i, (src, dst) in enumerate(((x, x_cols), (dy, dy_cols)))
        ]

    load_wd = pltpu.make_async_copy(w_down, wd, w_sem.at[0])
    def load_w(i):
        at = pl.ds(pl.multiple_of(lax.rem(q1 + turn(i), n) * block, 128), block)
        return [
            pltpu.make_async_copy(w_gate.at[at, :], wgu.at[at, pl.ds(0, ff)], w_sem.at[i, 0]),
            pltpu.make_async_copy(w_up.at[at, :], wgu.at[at, pl.ds(ff, ff)], w_sem.at[i, 1]),
        ]

    def split_grads(b, d_hidden):
        slot, at = lax.rem(b, 2), rows_of(b)
        g, u = g_rows[slot].astype(F32), u_rows[slot].astype(F32)
        sig = jax.nn.sigmoid(g)
        silu = g * sig
        dgu[pl.ds(at, HALF), pl.ds(0, ff)] = (d_hidden * u * (sig + silu * (1.0 - sig))).astype(BF16)
        dgu[pl.ds(at, HALF), pl.ds(ff, ff)] = (d_hidden * silu).astype(BF16)
        hid[:, pl.ds(at, HALF)] = (silu * u).T.astype(BF16)

    @scoped
    def hidden_grads(b):
        for copy in row_copies(b):
            copy.wait()
        split_grads(b, dot(dy_rows[lax.rem(b, 2)], wd[...], NT))

        @pl.when(b + 2 < 2 * chunks)
        def _():
            for copy in row_copies(b + 2):
                copy.start()

    def first_copies(i):
        at = pl.ds(i * (width // PIECES), width // PIECES)
        return [
            pltpu.make_async_copy(dy.at[pl.ds(rows_of(0), HALF), at], dy_rows.at[0, :, at], first_sem.at[i, 0]),
            pltpu.make_async_copy(w_down.at[:, at], wd.at[:, at], first_sem.at[i, 1]),
        ]

    @scoped
    def first_grads():
        behind = [load_w(0), row_copies(1), load_w(1), load_w(2) + load_w(3)]
        d_hidden = None
        for i in range(PIECES):
            for copy in first_copies(i):
                copy.wait()
            for copy in behind[i]:
                copy.start()
            at = pl.ds(i * (width // PIECES), width // PIECES)
            part = dot(dy_rows[0, :, at], wd[:, at], NT)
            d_hidden = part if d_hidden is None else d_hidden + part
        for copy in row_copies(0, first=1):
            copy.wait()
        split_grads(0, d_hidden)
        for copy in row_copies(2):
            copy.start()

    def term(at, b):
        return dot(dgu[pl.ds(at, HALF), :], wgu[pl.ds(pl.multiple_of(b * block, 128), block), :], NT)

    @scoped
    def partner_block(k, o):
        @pl.when(jnp.logical_and(k == 0, o == 0))
        def _():
            for copy in load_w(0):
                copy.wait()

        @pl.when(jnp.logical_and(k == 0, o == 1))
        def _():
            for i in range(1, n):
                for copy in load_w(i):
                    copy.wait()

        pl.when(k > 0)(lambda: swap(k - 1, o).wait_send())
        outbox[o] = term(other(k), lax.rem(q1 + turn(o), n)).astype(BF16)
        swap(k, o).start()

    @scoped
    def own_block(k, o):
        pl.when(jnp.logical_and(k >= SLOTS, o == 0))(lambda: reduced(k - SLOTS))
        b = lax.rem(p1 + turn(o), n)
        t = term(own(k), b)
        swap_in(k, o).wait_recv()
        sums[lax.rem(k, SLOTS), b] = (t + mine[pl.ds(kept(k), HALF), pl.ds(cols(b), block)].astype(F32)).astype(BF16)
        pl.when(o == 0)(lambda: send(0, k, 0, 1))
        pl.when(o == 1)(lambda: send(0, k, 2))
        pl.when(o == 2)(lambda: send(0, k, 3))

    @scoped
    def weight_grads(u):
        for copy in col_copies(u):
            copy.wait()
        slot = lax.rem(u, 2)

        at = pl.ds(pl.multiple_of(u * COLS, COLS), COLS)
        wgu[at, :] = dot(x_cols[slot], dgu[...], TN).astype(BF16)
        wd[:, at] = dot(hid[...], dy_cols[slot], NN).astype(BF16)

        @pl.when(u + 2 < units)
        def _():
            for copy in col_copies(u + 2):
                copy.start()

    def add(dst, size, *srcs):
        step = 32

        @pl.loop(0, size // step)
        def _(r):
            at = pl.multiple_of(r * step, step)
            total = srcs[0](at, step).astype(F32)
            for s in srcs[1:]:
                total = total + s(at, step).astype(F32)
            dst(at, step, total.astype(BF16))

    def add_sums(k, b, off, size, lanes, *lands):
        def mine(at, step):
            return sums[lax.rem(k, SLOTS), b, pl.ds(off + at, step), lanes]

        def put(at, step, v):
            sums[lax.rem(k, SLOTS), b, pl.ds(off + at, step), lanes] = v

        add(put, size, mine, *lands)

    def landed(row, first, wide):
        return lambda at, step: theirs[pl.ds(row + at, step), pl.ds(first, wide)]

    @scoped
    def s1(k):
        arrive(0, k, 0)
        add_sums(k, mod(p1 + n - 1), 0, hr, slice(None), landed(kept(k), 0, block))
        send(0, k, 4)
        arrive(0, k, 1)
        add_sums(k, mod(p1 + 1), hr, hr, slice(None), landed(kept(k) + hr, 0, block))
        send(0, k, 5)

    @scoped
    def s2(k):
        arrive(0, k, 2, 3, 4, 5)
        add_sums(k, p1, 0, HALF, slice(None), landed(kept(k), block, block), landed(kept(k), 2 * block, block))
        send(1, k, 0, 1, 2, 3)

    @scoped
    def s3(k):
        base = 3 * block
        arrive(1, k, 0)
        add_sums(k, p1, pl.multiple_of(mod(p2 + n - 1) * sub, sub), sub, pl.ds(0, hc), landed(kept(k), base, hc))
        send(1, k, 4)
        arrive(1, k, 1)
        add_sums(k, p1, pl.multiple_of(mod(p2 + 1) * sub, sub), sub, pl.ds(hc, hc), landed(kept(k), base + hc, hc))
        send(1, k, 5)

    @scoped
    def s4(k):
        arrive(1, k, 2, 3, 4, 5)
        off = pl.multiple_of(p2 * sub, sub)

        def put(at, step, v):
            mine[pl.ds(kept(k) + off + at, step), pl.ds(cols(p1), block)] = v

        add(
            put, sub,
            lambda at, step: sums[lax.rem(k, SLOTS), p1, pl.ds(off + at, step), :],
            landed(kept(k) + sub, 3 * block, block),
            landed(kept(k) + 2 * sub, 3 * block, block),
        )
        send(2, k, 0, 1, 2, 3)
        pl.semaphore_signal(credit.at[k], inc=1, device_id={"tp": partner}, device_id_type=MESH)

    @scoped
    def s5(k):
        arrive(2, k, 0)
        send(2, k, 4)
        arrive(2, k, 1)
        send(2, k, 5)

    @scoped
    def s6(k):
        arrive(2, k, 2, 3, 4, 5)
        send(3, k, 0, 1, 2, 3)
        pl.semaphore_wait(credit.at[k], 1)
        share(k, 0).start()

    @scoped
    def s7(k):
        arrive(3, k, 0)
        send(3, k, 4)
        arrive(3, k, 1)
        send(3, k, 5)

    @scoped
    def s8(k):
        arrive(3, k, 2)
        share(k, 1).start()
        arrive(3, k, 3)
        share(k, 2).start()
        arrive(3, k, 4)
        share(k, 3).start()
        arrive(3, k, 5)
        share(k, 4).start()

    @scoped
    def s9(k):
        for i in range(5):
            share_in(k, i).wait_recv()

    def matmuls(t):
        k, r = t // PERIOD, lax.rem(t, PERIOD)
        first = r < 4
        even = lax.rem(r, 2) == 0
        to_partner = jnp.logical_or(r == 1, jnp.logical_or(r == 3, jnp.logical_or(r == 5, r == 7)))
        to_own = jnp.logical_or(r == 4, jnp.logical_or(r == 6, r >= 8))
        grads = jnp.logical_and(first, even)
        pl.when(jnp.logical_and(grads, t > 0))(lambda: hidden_grads(2 * k + r // 2))
        pl.when(to_partner)(lambda: partner_block(k, r // 2))
        pl.when(to_own)(lambda: own_block(k, r // 6 + r // 8 + r // 9))

    stages = (s1, s2, s3, s4, s5, s6, s7, s8, s9)
    work = chunks * PERIOD

    barrier = pltpu.get_barrier_semaphore()
    for to in (left1, right1, left2, right2, partner):
        pl.semaphore_signal(barrier, inc=1, device_id={"tp": to}, device_id_type=MESH)
    for i in range(PIECES):
        for copy in first_copies(i):
            copy.start()
    for copy in row_copies(0, first=1):
        copy.start()
    first_grads()
    with jax.named_scope("meet"):
        pl.semaphore_wait(barrier, 5)

    @pl.loop(0, TICKS[-1][-1] + 1)
    def _(t):
        pl.when(t < work)(lambda: matmuls(t))

        @pl.when(t == PERIOD)
        def _():
            for u in range(2):
                for copy in col_copies(u):
                    copy.start()

        pl.when(jnp.logical_and(t >= work, t < work + units))(lambda: weight_grads(t - work))
        for stage, ticks in zip(stages, TICKS):
            now, k = t == ticks[0], 0
            for tick in ticks[1:]:
                now = jnp.logical_or(now, t == tick)
                k = k + (t >= tick).astype(jnp.int32)
            pl.when(now)(functools.partial(stage, k))

    @pl.loop(0, chunks)
    def _(k):
        pl.when(k >= chunks - SLOTS)(lambda: reduced(k))
        for phase in (2, 3):
            for i in range(6):
                ring(phase, k, i).wait_send()
        for i in range(5):
            share(k, i).wait_send()

    @pl.loop(0, n)
    def _(o):
        swap(chunks - 1, o).wait_send()


def store(dw_gu, dw_d, mine, theirs, dx, dw_gate, dw_up, dw_down, sem):
    c = lax.rem(lax.axis_index("tp"), 2)
    ff = dw_gate.shape[1]
    pairs = [(dw_gu.at[:, pl.ds(0, ff)], dw_gate), (dw_gu.at[:, pl.ds(ff, ff)], dw_up), (dw_d, dw_down)]
    for k in range(mine.shape[0] // HALF):
        for half, core in ((mine, c), (theirs, 1 - c)):
            at = pl.ds(pl.multiple_of((2 * k + core) * HALF, HALF), HALF)
            pairs.append((half.at[pl.ds(k * HALF, HALF), :], dx.at[at, :]))
    copies = [pltpu.make_async_copy(src, dst, sem.at[i]) for i, (src, dst) in enumerate(pairs)]
    for copy in copies:
        copy.start()
    for copy in copies:
        copy.wait()


def solution(mesh):
    n = math.isqrt(mesh.shape["tp"] // 2)
    if n != 4 or 2 * n * n != mesh.shape["tp"]:
        raise ValueError("unexpected group")

    def step(x, dy, gate, up, w_gate, w_up, w_down):
        rows, width = x.shape
        ff = gate.shape[1]
        chunks, block = rows // (2 * HALF), width // n
        any_space = pl.BlockSpec(memory_space=pl.ANY)
        vmem = pl.BlockSpec(memory_space=pltpu.VMEM)
        dma = pltpu.SemaphoreType.DMA
        kept = pl.pallas_call(
            functools.partial(kernel, n),
            out_shape=(
                pltpu.VMEM((width, 2 * ff), BF16),
                pltpu.VMEM((ff, width), BF16),
                pltpu.VMEM((rows // 2, width), BF16),
                pltpu.VMEM((rows // 2, width), BF16),
            ),
            in_specs=[any_space] * 7,
            out_specs=[vmem] * 4,
            scratch_shapes=[
                pltpu.VMEM((rows, 2 * ff), BF16),
                pltpu.VMEM((ff, rows), BF16),
                pltpu.VMEM((SLOTS, n, HALF, block), BF16),
                pltpu.VMEM((n, HALF, block), BF16),
                pltpu.VMEM((2, HALF, width), BF16),
                pltpu.VMEM((2, HALF, ff), BF16),
                pltpu.VMEM((2, HALF, ff), BF16),
                pltpu.VMEM((2, rows, COLS), BF16),
                pltpu.VMEM((2, rows, COLS), BF16),
                dma((chunks, 4, 6)),
                dma((chunks, 4, 6)),
                dma((chunks, n + 5)),
                dma((chunks, n + 5)),
                pltpu.SemaphoreType.REGULAR((chunks,)),
                dma((n, 2)),
                dma((PIECES, 2)),
                dma((2, 3)),
                dma((2, 2)),
            ],
            compiler_params=pltpu.CompilerParams(
                collective_id=0, has_side_effects=True, vmem_limit_bytes=31 * 1024 * 1024
            ),
        )(x, dy, gate, up, w_gate, w_up, w_down)
        return pl.pallas_call(
            store,
            out_shape=[jax.ShapeDtypeStruct(a.shape, BF16) for a in (x, w_gate, w_up, w_down)],
            in_specs=[vmem] * 4,
            out_specs=[any_space] * 4,
            scratch_shapes=[dma((3 + rows // HALF,))],
            compiler_params=pltpu.CompilerParams(vmem_limit_bytes=1024 * 1024),
        )(*kept)

    tokens, columns, by_rows = P("dp", None), P(None, "tp"), P("tp", None)
    return jax.shard_map(
        step,
        mesh=mesh,
        in_specs=(tokens, tokens, P("dp", "tp"), P("dp", "tp"), columns, columns, by_rows),
        out_specs=(tokens, P("dp", "tp"), P("dp", "tp"), P(("dp", "tp"), None)),
        check_vma=False,
    )
```

```python
import functools
import math

import jax
import jax.numpy as jnp
from jax import lax
from jax.experimental import pallas as pl
from jax.experimental.pallas import tpu as pltpu
from jax.sharding import PartitionSpec as P

MESH = pl.DeviceIdType.MESH
HALF = 256
SLOTS = 3
PERIOD = 10
TICKS = (
    (10, 20, 30, 40),
    (17, 27, 37, 45),
    (21, 31, 41, 48),
    (25, 35, 44, 51),
    (29, 39, 47, 54),
    (41, 45, 52, 57),
    (48, 54, 60, 64),
    (54, 60, 65, 70),
    (58, 64, 70, 75),
)
PIECES = 4
COLS = 256
F32, BF16 = jnp.float32, jnp.bfloat16
NT = (((1,), (1,)), ((), ()))
TN = (((0,), (0,)), ((), ()))
NN = (((1,), (0,)), ((), ()))


def dot(a, b, dims):
    return lax.dot_general(a, b, dims, preferred_element_type=F32)


def scoped(stage):
    def named(*args):
        with jax.named_scope(stage.__name__):
            return stage(*args)

    return named


def kernel(
    n, x, dy, gate, up, w_gate, w_up, w_down,
    wgu, wd, mine, theirs,
    dgu, hid, sums, outbox, dy_rows, g_rows, u_rows, x_cols, dy_cols,
    ring_send, ring_recv, swap_send, share_send, pair_recv, credit, w_sem, first_sem, row_sem, col_sem,
):
    rows, width = x.shape
    ff = gate.shape[1]
    chunks = rows // (2 * HALF)
    block = width // n
    sub = HALF // n
    hr, hc = HALF // 2, block // 2
    units = width // COLS

    me = lax.axis_index("tp")
    c = lax.rem(me, 2)
    chip = me // 2
    px, py = chip // n, lax.rem(chip, n)
    p1 = px * (1 - c) + py * c
    p2 = py * (1 - c) + px * c

    def device(ax, ay, core):
        return (lax.rem(ax, n) * n + lax.rem(ay, n)) * 2 + core

    sx, sy = 1 - c, c
    right1, left1 = device(px + sx, py + sy, c), device(px + n - sx, py + n - sy, c)
    right2, left2 = device(px + sy, py + sx, c), device(px + n - sy, py + n - sx, c)
    partner = device(px, py, 1 - c)
    q1 = px * c + py * (1 - c)

    def mod(v):
        return lax.rem(v + n, n)

    def own(k):
        return pl.multiple_of((2 * k + c) * HALF, HALF)

    def other(k):
        return pl.multiple_of((2 * k + 1 - c) * HALF, HALF)

    def turn(o):
        return (2 + o) * (1 - o // 2) + (3 - o) * (o // 2)

    def kept(k):
        return pl.multiple_of(k * HALF, HALF)

    def cols(b):
        return pl.multiple_of(b * block, 128)

    def remote(src, dst, ssem, rsem, to):
        return pltpu.make_async_remote_copy(
            src_ref=src, dst_ref=dst, send_sem=ssem, recv_sem=rsem, device_id={"tp": to}, device_id_type=MESH
        )

    def rs1_src(k, b, h):
        return sums.at[lax.rem(k, SLOTS), b, pl.ds(h * hr, hr), :]

    def rs1_land(k, area, h):
        return theirs.at[pl.ds(kept(k) + h * hr, hr), pl.ds(area * block, block)]

    def rs2_src(k, s, h):
        return sums.at[lax.rem(k, SLOTS), p1, pl.ds(pl.multiple_of(s * sub, sub), sub), pl.ds(h * hc, hc)]

    def rs2_land(k, area, h):
        return theirs.at[pl.ds(kept(k) + area * sub, sub), pl.ds(3 * block + h * hc, hc)]

    def ag2_at(k, s, h):
        return mine.at[pl.ds(kept(k) + pl.multiple_of(s * sub, sub), sub), pl.ds(cols(p1) + h * hc, hc)]

    late = (0, 1, n - 1, 2)

    def ag1_at(k, b, o):
        at = pl.multiple_of(mod(p2 + late[o]) * sub, sub)
        return mine.at[pl.ds(kept(k) + at, sub), pl.ds(cols(b), block)]

    arrivals = (
        (0, 1, 2, 2, 2, 2),
        (3, 4, 5, 5, 5, 5),
        (6, 7, 8, 9, 10, 10),
        (11, 16, 13, 16, 15, 12, 15, 14, 17, 18, 19, 20),
    )

    def together(ref, ssem, rsem):
        return remote(ref, ref, ssem, rsem, partner)

    def arrive_together(phase, k, i, ref):
        together(ref, ring_send.at[k, phase], ring_recv.at[k, arrivals[phase][i]]).wait_recv()

    def left_together(phase, k, ref):
        together(ref, ring_send.at[k, phase], ring_recv.at[k, 0]).wait_send()

    land = {0: (0, 0), 1: (0, 1), 2: (1, 1), 3: (2, 0), 4: (1, 0), 5: (2, 1)}

    def reduce_pair(src, dst, p, i):
        which = {0: (2, 0), 1: (2, 1), 2: (n - 1, 1), 3: (1, 0), 4: (n - 1, 0), 5: (1, 1)}[i]
        return src(mod(p + which[0]), which[1]), dst(*land[i])

    def gather_at(at, p, i, arriving):
        off, h = {0: (0, 0), 1: (0, 1), 2: (0, 1), 3: (0, 0), 4: (1, 0), 5: (n - 1, 1)}[i]
        step = (1 if i % 2 == 0 else n - 1) if arriving else 0
        return at(mod(p + off + step), h)

    def ring(phase, k, i, arriving=False):
        left, right = (left1, right1) if phase in (0, 3) else (left2, right2)
        if phase == 0:
            src, dst = reduce_pair(functools.partial(rs1_src, k), functools.partial(rs1_land, k), p1, i)
        elif phase == 1:
            src, dst = reduce_pair(functools.partial(rs2_src, k), functools.partial(rs2_land, k), p2, i)
        elif phase == 2:
            src = dst = gather_at(functools.partial(ag2_at, k), p2, i, arriving)
        else:
            o, off = (i // 2, 0) if i < 8 else (i // 2 - 4 + 2 * (i % 2), (1, n - 1)[i % 2])
            src = dst = ag1_at(k, mod(p1 + off + ((1, n - 1)[i % 2] if arriving else 0)), o)
        to = left if i % 2 == 0 else right
        return remote(src, dst, ring_send.at[k, phase], ring_recv.at[k, arrivals[phase][i]], to)

    def send(phase, k, *which):
        for i in which:
            ring(phase, k, i).start()

    def arrive(phase, k, *which):
        for i in which:
            ring(phase, k, i, arriving=True).wait_recv()

    def reduced(k):
        left_together(0, k, sums.at[lax.rem(k, SLOTS), pl.ds(0, 3)])
        left_together(1, k, sums.at[lax.rem(k, SLOTS), 0, pl.ds(0, 3 * sub), :])

    def swap(k, o):
        b = lax.rem(q1 + turn(o), n)
        return remote(
            outbox.at[o], mine.at[pl.ds(kept(k), HALF), pl.ds(cols(b), block)],
            swap_send.at[o], pair_recv.at[k, o], partner,
        )

    def swap_in(k, o):
        b = lax.rem(p1 + turn(o), n)
        return remote(
            outbox.at[o], mine.at[pl.ds(kept(k), HALF), pl.ds(cols(b), block)],
            swap_send.at[o], pair_recv.at[k, o], partner,
        )

    def shared(k, i, place, piece):
        b = mod(place + (0, 1, n - 1, 2, 2, 2, 2)[i])
        if i < 3:
            return pl.ds(kept(k), HALF), pl.ds(cols(b), block)
        at = pl.multiple_of(mod(piece + late[i - 3]) * sub, sub)
        return pl.ds(kept(k) + at, sub), pl.ds(cols(b), block)

    def share(k, i):
        at = shared(k, i, p1, p2)
        return remote(mine.at[at], theirs.at[at], share_send.at[k], pair_recv.at[k, n], partner)

    def rows_of(b):
        return pl.multiple_of((2 * (b // 2) + lax.rem(b + 1 + c, 2)) * HALF, HALF)

    def row_copies(b, first=0):
        at = pl.ds(rows_of(b), HALF)
        slot = lax.rem(b, 2)
        pairs = ((dy, dy_rows), (gate, g_rows), (up, u_rows))
        return [
            pltpu.make_async_copy(pairs[i][0].at[at, :], pairs[i][1].at[slot], row_sem.at[slot, i]) for i in range(first, 3)
        ]

    def col_copies(u):
        at = pl.ds(pl.multiple_of(u * COLS, COLS), COLS)
        slot = lax.rem(u, 2)
        return [
            pltpu.make_async_copy(src.at[:, at], dst.at[slot], col_sem.at[slot, i])
            for i, (src, dst) in enumerate(((x, x_cols), (dy, dy_cols)))
        ]

    load_wd = pltpu.make_async_copy(w_down, wd, w_sem.at[0])
    def load_w(i):
        at = pl.ds(pl.multiple_of(lax.rem(q1 + turn(i), n) * block, 128), block)
        return [
            pltpu.make_async_copy(w_gate.at[at, :], wgu.at[at, pl.ds(0, ff)], w_sem.at[i, 0]),
            pltpu.make_async_copy(w_up.at[at, :], wgu.at[at, pl.ds(ff, ff)], w_sem.at[i, 1]),
        ]

    def split_grads(b, d_hidden):
        slot, at = lax.rem(b, 2), rows_of(b)
        g, u = g_rows[slot].astype(F32), u_rows[slot].astype(F32)
        sig = jax.nn.sigmoid(g)
        silu = g * sig
        dgu[pl.ds(at, HALF), pl.ds(0, ff)] = (d_hidden * u * (sig + silu * (1.0 - sig))).astype(BF16)
        dgu[pl.ds(at, HALF), pl.ds(ff, ff)] = (d_hidden * silu).astype(BF16)
        hid[:, pl.ds(at, HALF)] = (silu * u).T.astype(BF16)

    @scoped
    def hidden_grads(b):
        for copy in row_copies(b):
            copy.wait()
        split_grads(b, dot(dy_rows[lax.rem(b, 2)], wd[...], NT))

        @pl.when(b + 2 < 2 * chunks)
        def _():
            for copy in row_copies(b + 2):
                copy.start()

    def first_copies(i):
        at = pl.ds(i * (width // PIECES), width // PIECES)
        return [
            pltpu.make_async_copy(dy.at[pl.ds(rows_of(0), HALF), at], dy_rows.at[0, :, at], first_sem.at[i, 0]),
            pltpu.make_async_copy(w_down.at[:, at], wd.at[:, at], first_sem.at[i, 1]),
        ]

    @scoped
    def first_grads():
        behind = [load_w(0), row_copies(1), load_w(1), load_w(2) + load_w(3)]
        d_hidden = None
        for i in range(PIECES):
            for copy in first_copies(i):
                copy.wait()
            for copy in behind[i]:
                copy.start()
            at = pl.ds(i * (width // PIECES), width // PIECES)
            part = dot(dy_rows[0, :, at], wd[:, at], NT)
            d_hidden = part if d_hidden is None else d_hidden + part
        for copy in row_copies(0, first=1):
            copy.wait()
        split_grads(0, d_hidden)
        for copy in row_copies(2):
            copy.start()

    def term(at, b):
        return dot(dgu[pl.ds(at, HALF), :], wgu[pl.ds(pl.multiple_of(b * block, 128), block), :], NT)

    @scoped
    def partner_block(k, o):
        @pl.when(jnp.logical_and(k == 0, o == 0))
        def _():
            for copy in load_w(0):
                copy.wait()

        @pl.when(jnp.logical_and(k == 0, o == 1))
        def _():
            for i in range(1, n):
                for copy in load_w(i):
                    copy.wait()

        pl.when(k > 0)(lambda: swap(k - 1, o).wait_send())
        outbox[o] = term(other(k), lax.rem(q1 + turn(o), n)).astype(BF16)
        swap(k, o).start()

    @scoped
    def own_block(k, o):
        pl.when(jnp.logical_and(k >= SLOTS, o == 0))(lambda: reduced(k - SLOTS))
        b = lax.rem(p1 + turn(o), n)
        t = term(own(k), b)
        swap_in(k, o).wait_recv()
        sums[lax.rem(k, SLOTS), b] = (t + mine[pl.ds(kept(k), HALF), pl.ds(cols(b), block)].astype(F32)).astype(BF16)
        pl.when(o == 0)(lambda: send(0, k, 0, 1))
        pl.when(o == 1)(lambda: send(0, k, 2))
        pl.when(o == 2)(lambda: send(0, k, 3))

    @scoped
    def weight_grads(u):
        for copy in col_copies(u):
            copy.wait()
        slot = lax.rem(u, 2)

        at = pl.ds(pl.multiple_of(u * COLS, COLS), COLS)
        wgu[at, :] = dot(x_cols[slot], dgu[...], TN).astype(BF16)
        wd[:, at] = dot(hid[...], dy_cols[slot], NN).astype(BF16)

        @pl.when(u + 2 < units)
        def _():
            for copy in col_copies(u + 2):
                copy.start()

    def add(dst, size, *srcs):
        step = 32

        @pl.loop(0, size // step)
        def _(r):
            at = pl.multiple_of(r * step, step)
            total = srcs[0](at, step).astype(F32)
            for s in srcs[1:]:
                total = total + s(at, step).astype(F32)
            dst(at, step, total.astype(BF16))

    def add_sums(k, b, off, size, lanes, *lands):
        def mine(at, step):
            return sums[lax.rem(k, SLOTS), b, pl.ds(off + at, step), lanes]

        def put(at, step, v):
            sums[lax.rem(k, SLOTS), b, pl.ds(off + at, step), lanes] = v

        add(put, size, mine, *lands)

    def landed(row, first, wide):
        return lambda at, step: theirs[pl.ds(row + at, step), pl.ds(first, wide)]

    @scoped
    def s1(k):
        @pl.when(k == chunks - 1)
        def _():
            for o in range(n):
                swap(k, o).wait_send()

        arrive(0, k, 0)
        add_sums(k, mod(p1 + n - 1), 0, hr, slice(None), landed(kept(k), 0, block))
        send(0, k, 4)
        arrive(0, k, 1)
        add_sums(k, mod(p1 + 1), hr, hr, slice(None), landed(kept(k) + hr, 0, block))
        send(0, k, 5)

    @scoped
    def s2(k):
        arrive_together(0, k, 2, theirs.at[pl.ds(kept(k), HALF), pl.ds(block, 2 * block)])
        add_sums(k, p1, 0, HALF, slice(None), landed(kept(k), block, block), landed(kept(k), 2 * block, block))
        send(1, k, 0, 1, 2, 3)

    @scoped
    def s3(k):
        base = 3 * block
        arrive(1, k, 0)
        add_sums(k, p1, pl.multiple_of(mod(p2 + n - 1) * sub, sub), sub, pl.ds(0, hc), landed(kept(k), base, hc))
        send(1, k, 4)
        arrive(1, k, 1)
        add_sums(k, p1, pl.multiple_of(mod(p2 + 1) * sub, sub), sub, pl.ds(hc, hc), landed(kept(k), base + hc, hc))
        send(1, k, 5)

    @scoped
    def s4(k):
        arrive_together(1, k, 2, theirs.at[pl.ds(kept(k) + sub, 2 * sub), pl.ds(3 * block, block)])
        off = pl.multiple_of(p2 * sub, sub)

        def put(at, step, v):
            mine[pl.ds(kept(k) + off + at, step), pl.ds(cols(p1), block)] = v

        add(
            put, sub,
            lambda at, step: sums[lax.rem(k, SLOTS), p1, pl.ds(off + at, step), :],
            landed(kept(k) + sub, 3 * block, block),
            landed(kept(k) + 2 * sub, 3 * block, block),
        )
        send(2, k, 0, 1, 2, 3)
        pl.when(k == chunks - 1)(lambda: send(3, k, 0, 1))
        pl.semaphore_signal(credit.at[k], inc=1, device_id={"tp": partner}, device_id_type=MESH)

    @scoped
    def s5(k):
        arrive(2, k, 0)
        send(2, k, 4)
        arrive(2, k, 1)
        send(2, k, 5)

    @scoped
    def s6(k):
        pl.when(k < chunks - 1)(lambda: send(3, k, 0, 1))
        arrive(2, k, 2)
        send(3, k, 2)
        arrive(2, k, 3)
        send(3, k, 4, 5)
        arrive_together(2, k, 4, mine.at[pl.ds(kept(k), sub), pl.ds(cols(p1), block)])
        send(3, k, 6, 7, 3)
        pl.semaphore_wait(credit.at[k], 1)
        share(k, 0).start()

    @scoped
    def s7(k):
        for came, on in ((0, 8), (5, 9), (2, 10), (7, 11)):
            arrive(3, k, came)
            send(3, k, on)

    @scoped
    def s8(k):
        pl.when(k >= chunks - SLOTS)(lambda: reduced(k))
        left_together(2, k, mine.at[pl.ds(kept(k), 3 * sub), pl.ds(0, block)])
        arrive_together(3, k, 4, mine.at[pl.ds(kept(k), hr), pl.ds(cols(mod(p1 + 1)), block)])
        share(k, 1).start()
        arrive_together(3, k, 1, mine.at[pl.ds(kept(k), hr), pl.ds(cols(mod(p1 + n - 1)), block)])
        share(k, 2).start()
        for came, i in ((8, 3), (9, 5), (10, 4), (11, 6)):
            arrive(3, k, came)
            share(k, i).start()

    @scoped
    def s9(k):
        whole = pl.ds(kept(k), HALF)
        together(theirs.at[whole, :], share_send.at[k], pair_recv.at[k, n]).wait_recv()
        left_together(3, k, sums.at[lax.rem(k, SLOTS), pl.ds(0, 3)])
        together(mine.at[whole, :], share_send.at[k], pair_recv.at[k, n]).wait_send()

    def matmuls(t):
        k, r = t // PERIOD, lax.rem(t, PERIOD)
        first = r < 4
        even = lax.rem(r, 2) == 0
        to_partner = jnp.logical_or(r == 1, jnp.logical_or(r == 3, jnp.logical_or(r == 5, r == 7)))
        to_own = jnp.logical_or(r == 4, jnp.logical_or(r == 6, r >= 8))
        grads = jnp.logical_and(first, even)
        pl.when(jnp.logical_and(grads, t > 0))(lambda: hidden_grads(2 * k + r // 2))
        pl.when(to_partner)(lambda: partner_block(k, r // 2))
        pl.when(to_own)(lambda: own_block(k, r // 6 + r // 8 + r // 9))

    stages = (s1, s2, s3, s4, s5, s6, s7, s8, s9)
    work = chunks * PERIOD

    barrier = pltpu.get_barrier_semaphore()
    for to in (left1, right1, left2, right2, partner):
        pl.semaphore_signal(barrier, inc=1, device_id={"tp": to}, device_id_type=MESH)
    for i in range(PIECES):
        for copy in first_copies(i):
            copy.start()
    for copy in row_copies(0, first=1):
        copy.start()
    first_grads()
    with jax.named_scope("meet"):
        pl.semaphore_wait(barrier, 5)

    @pl.loop(0, TICKS[-1][-1] + 1)
    def _(t):
        pl.when(t < work)(lambda: matmuls(t))

        @pl.when(t == PERIOD)
        def _():
            for u in range(2):
                for copy in col_copies(u):
                    copy.start()

        pl.when(jnp.logical_and(t >= work, t < work + units))(lambda: weight_grads(t - work))
        for stage, ticks in zip(stages, TICKS):
            now, k = t == ticks[0], 0
            for tick in ticks[1:]:
                now = jnp.logical_or(now, t == tick)
                k = k + (t >= tick).astype(jnp.int32)
            pl.when(now)(functools.partial(stage, k))


def store(dw_gu, dw_d, mine, theirs, dx, dw_gate, dw_up, dw_down, sem):
    c = lax.rem(lax.axis_index("tp"), 2)
    ff = dw_gate.shape[1]
    pairs = [(dw_gu.at[:, pl.ds(0, ff)], dw_gate), (dw_gu.at[:, pl.ds(ff, ff)], dw_up), (dw_d, dw_down)]
    for k in range(mine.shape[0] // HALF):
        for half, core in ((mine, c), (theirs, 1 - c)):
            at = pl.ds(pl.multiple_of((2 * k + core) * HALF, HALF), HALF)
            pairs.append((half.at[pl.ds(k * HALF, HALF), :], dx.at[at, :]))
    copies = [pltpu.make_async_copy(src, dst, sem.at[i]) for i, (src, dst) in enumerate(pairs)]
    for copy in copies:
        copy.start()
    for copy in copies:
        copy.wait()


def solution(mesh):
    n = math.isqrt(mesh.shape["tp"] // 2)
    if n != 4 or 2 * n * n != mesh.shape["tp"]:
        raise ValueError("unexpected group")

    def step(x, dy, gate, up, w_gate, w_up, w_down):
        rows, width = x.shape
        ff = gate.shape[1]
        chunks, block = rows // (2 * HALF), width // n
        any_space = pl.BlockSpec(memory_space=pl.ANY)
        vmem = pl.BlockSpec(memory_space=pltpu.VMEM)
        dma = pltpu.SemaphoreType.DMA
        kept = pl.pallas_call(
            functools.partial(kernel, n),
            out_shape=(
                pltpu.VMEM((width, 2 * ff), BF16),
                pltpu.VMEM((ff, width), BF16),
                pltpu.VMEM((rows // 2, width), BF16),
                pltpu.VMEM((rows // 2, width), BF16),
            ),
            in_specs=[any_space] * 7,
            out_specs=[vmem] * 4,
            scratch_shapes=[
                pltpu.VMEM((rows, 2 * ff), BF16),
                pltpu.VMEM((ff, rows), BF16),
                pltpu.VMEM((SLOTS, n, HALF, block), BF16),
                pltpu.VMEM((n, HALF, block), BF16),
                pltpu.VMEM((2, HALF, width), BF16),
                pltpu.VMEM((2, HALF, ff), BF16),
                pltpu.VMEM((2, HALF, ff), BF16),
                pltpu.VMEM((2, rows, COLS), BF16),
                pltpu.VMEM((2, rows, COLS), BF16),
                dma((chunks, 4)),
                dma((chunks, 21)),
                dma((n,)),
                dma((chunks,)),
                dma((chunks, n + 1)),
                pltpu.SemaphoreType.REGULAR((chunks,)),
                dma((n, 2)),
                dma((PIECES, 2)),
                dma((2, 3)),
                dma((2, 2)),
            ],
            compiler_params=pltpu.CompilerParams(
                collective_id=0, has_side_effects=True, vmem_limit_bytes=31 * 1024 * 1024
            ),
        )(x, dy, gate, up, w_gate, w_up, w_down)
        return pl.pallas_call(
            store,
            out_shape=[jax.ShapeDtypeStruct(a.shape, BF16) for a in (x, w_gate, w_up, w_down)],
            in_specs=[vmem] * 4,
            out_specs=[any_space] * 4,
            scratch_shapes=[dma((3 + rows // HALF,))],
            compiler_params=pltpu.CompilerParams(vmem_limit_bytes=1024 * 1024),
        )(*kept)

    tokens, columns, by_rows = P("dp", None), P(None, "tp"), P("tp", None)
    return jax.shard_map(
        step,
        mesh=mesh,
        in_specs=(tokens, tokens, P("dp", "tp"), P("dp", "tp"), columns, columns, by_rows),
        out_specs=(tokens, P("dp", "tp"), P("dp", "tp"), P(("dp", "tp"), None)),
        check_vma=False,
    )
```

```python
import functools
import math

import jax
import jax.numpy as jnp
from jax import lax
from jax.experimental import pallas as pl
from jax.experimental.pallas import tpu as pltpu
from jax.sharding import PartitionSpec as P

MESH = pl.DeviceIdType.MESH
HALF = 256
SLOTS = 3
PERIOD = 10
TICKS = (
    (10, 20, 30, 40),
    (17, 27, 37, 45),
    (21, 31, 41, 48),
    (25, 35, 44, 51),
    (29, 39, 47, 54),
    (41, 45, 52, 57),
    (48, 54, 60, 64),
    (54, 60, 65, 70),
    (58, 64, 70, 75),
)
PIECES = 4
COLS = 256
F32, BF16 = jnp.float32, jnp.bfloat16
NT = (((1,), (1,)), ((), ()))
TN = (((0,), (0,)), ((), ()))
NN = (((1,), (0,)), ((), ()))


def dot(a, b, dims):
    return lax.dot_general(a, b, dims, preferred_element_type=F32)


def scoped(stage):
    def named(*args):
        with jax.named_scope(stage.__name__):
            return stage(*args)

    return named


def kernel(
    n, x, dy, gate, up, w_gate, w_up, w_down,
    wgu, wd, mine, theirs,
    dgu, hid, sums, outbox, dy_rows, g_rows, u_rows, x_cols, dy_cols,
    ring_send, ring_recv, swap_send, share_send, pair_recv, credit, w_sem, first_sem, row_sem, col_sem,
):
    rows, width = x.shape
    ff = gate.shape[1]
    chunks = rows // (2 * HALF)
    block = width // n
    sub = HALF // n
    hr, hc = HALF // 2, block // 2
    units = width // COLS

    me = lax.axis_index("tp")
    c = lax.rem(me, 2)
    chip = me // 2
    px, py = chip // n, lax.rem(chip, n)
    p1 = px * (1 - c) + py * c
    p2 = py * (1 - c) + px * c

    def device(ax, ay, core):
        return (lax.rem(ax, n) * n + lax.rem(ay, n)) * 2 + core

    sx, sy = 1 - c, c
    right1, left1 = device(px + sx, py + sy, c), device(px + n - sx, py + n - sy, c)
    right2, left2 = device(px + sy, py + sx, c), device(px + n - sy, py + n - sx, c)
    partner = device(px, py, 1 - c)
    q1 = px * c + py * (1 - c)

    def mod(v):
        return lax.rem(v + n, n)

    def own(k):
        return pl.multiple_of((2 * k + c) * HALF, HALF)

    def other(k):
        return pl.multiple_of((2 * k + 1 - c) * HALF, HALF)

    def turn(o):
        return (2 + o) * (1 - o // 2) + (3 - o) * (o // 2)

    def kept(k):
        return pl.multiple_of(k * HALF, HALF)

    def cols(b):
        return pl.multiple_of(b * block, 128)

    def remote(src, dst, ssem, rsem, to):
        return pltpu.make_async_remote_copy(
            src_ref=src, dst_ref=dst, send_sem=ssem, recv_sem=rsem, device_id={"tp": to}, device_id_type=MESH
        )

    def rs1_src(k, b, h):
        return sums.at[lax.rem(k, SLOTS), b, pl.ds(h * hr, hr), :]

    def rs1_land(k, area, h):
        return theirs.at[pl.ds(kept(k) + h * hr, hr), pl.ds(area * block, block)]

    def rs2_src(k, s, h):
        return sums.at[lax.rem(k, SLOTS), p1, pl.ds(pl.multiple_of(s * sub, sub), sub), pl.ds(h * hc, hc)]

    def rs2_land(k, area, h):
        return theirs.at[pl.ds(kept(k) + area * sub, sub), pl.ds(3 * block + h * hc, hc)]

    def ag2_at(k, s, h):
        return mine.at[pl.ds(kept(k) + pl.multiple_of(s * sub, sub), sub), pl.ds(cols(p1) + h * hc, hc)]

    late = (0, 1, n - 1, 2)

    def ag1_at(k, b, o):
        at = pl.multiple_of(mod(p2 + late[o]) * sub, sub)
        return mine.at[pl.ds(kept(k) + at, sub), pl.ds(cols(b), block)]

    arrivals = (
        (0, 1, 2, 2, 2, 2),
        (3, 4, 5, 5, 5, 5),
        (6, 7, 8, 9, 10, 10),
        (11, 16, 13, 16, 15, 12, 15, 14, 17, 18, 19, 20),
    )

    def together(ref, ssem, rsem):
        return remote(ref, ref, ssem, rsem, partner)

    def arrive_together(phase, k, i, ref):
        together(ref, ring_send.at[k, phase], ring_recv.at[k, arrivals[phase][i]]).wait_recv()

    def left_together(phase, k, ref):
        together(ref, ring_send.at[k, phase], ring_recv.at[k, 0]).wait_send()

    land = {0: (0, 0), 1: (0, 1), 2: (1, 1), 3: (2, 0), 4: (1, 0), 5: (2, 1)}

    def reduce_pair(src, dst, p, i):
        which = {0: (2, 0), 1: (2, 1), 2: (n - 1, 1), 3: (1, 0), 4: (n - 1, 0), 5: (1, 1)}[i]
        return src(mod(p + which[0]), which[1]), dst(*land[i])

    def gather_at(at, p, i, arriving):
        off, h = {0: (0, 0), 1: (0, 1), 2: (0, 1), 3: (0, 0), 4: (1, 0), 5: (n - 1, 1)}[i]
        step = (1 if i % 2 == 0 else n - 1) if arriving else 0
        return at(mod(p + off + step), h)

    def ring(phase, k, i, arriving=False):
        left, right = (left1, right1) if phase in (0, 3) else (left2, right2)
        if phase == 0:
            src, dst = reduce_pair(functools.partial(rs1_src, k), functools.partial(rs1_land, k), p1, i)
        elif phase == 1:
            src, dst = reduce_pair(functools.partial(rs2_src, k), functools.partial(rs2_land, k), p2, i)
        elif phase == 2:
            src = dst = gather_at(functools.partial(ag2_at, k), p2, i, arriving)
        else:
            o, off = (i // 2, 0) if i < 8 else (i // 2 - 4 + 2 * (i % 2), (1, n - 1)[i % 2])
            src = dst = ag1_at(k, mod(p1 + off + ((1, n - 1)[i % 2] if arriving else 0)), o)
        to = left if i % 2 == 0 else right
        return remote(src, dst, ring_send.at[k, phase], ring_recv.at[k, arrivals[phase][i]], to)

    def send(phase, k, *which):
        for i in which:
            ring(phase, k, i).start()

    def arrive(phase, k, *which):
        for i in which:
            ring(phase, k, i, arriving=True).wait_recv()

    def reduced(k):
        left_together(0, k, sums.at[lax.rem(k, SLOTS), pl.ds(0, 3)])
        left_together(1, k, sums.at[lax.rem(k, SLOTS), 0, pl.ds(0, 3 * sub), :])

    def swap(k, o):
        b = lax.rem(q1 + turn(o), n)
        return remote(
            outbox.at[o], mine.at[pl.ds(kept(k), HALF), pl.ds(cols(b), block)],
            swap_send.at[o], pair_recv.at[k, o], partner,
        )

    def swap_in(k, o):
        b = lax.rem(p1 + turn(o), n)
        return remote(
            outbox.at[o], mine.at[pl.ds(kept(k), HALF), pl.ds(cols(b), block)],
            swap_send.at[o], pair_recv.at[k, o], partner,
        )

    def shared(k, i, place, piece):
        b = mod(place + (0, 1, n - 1, 2, 2, 2, 2)[i])
        if i < 3:
            return pl.ds(kept(k), HALF), pl.ds(cols(b), block)
        at = pl.multiple_of(mod(piece + late[i - 3]) * sub, sub)
        return pl.ds(kept(k) + at, sub), pl.ds(cols(b), block)

    def share(k, i):
        at = shared(k, i, p1, p2)
        return remote(mine.at[at], theirs.at[at], share_send.at[k], pair_recv.at[k, n], partner)

    def rows_of(b):
        return pl.multiple_of((2 * (b // 2) + lax.rem(b + 1 + c, 2)) * HALF, HALF)

    def row_copies(b, first=0):
        at = pl.ds(rows_of(b), HALF)
        slot = lax.rem(b, 2)
        pairs = ((dy, dy_rows), (gate, g_rows), (up, u_rows))
        return [
            pltpu.make_async_copy(pairs[i][0].at[at, :], pairs[i][1].at[slot], row_sem.at[slot, i]) for i in range(first, 3)
        ]

    def col_copies(u):
        at = pl.ds(pl.multiple_of(u * COLS, COLS), COLS)
        slot = lax.rem(u, 2)
        return [
            pltpu.make_async_copy(src.at[:, at], dst.at[slot], col_sem.at[slot, i])
            for i, (src, dst) in enumerate(((x, x_cols), (dy, dy_cols)))
        ]

    load_wd = pltpu.make_async_copy(w_down, wd, w_sem.at[0])
    def load_w(i):
        at = pl.ds(pl.multiple_of(lax.rem(q1 + turn(i), n) * block, 128), block)
        return [
            pltpu.make_async_copy(w_gate.at[at, :], wgu.at[at, pl.ds(0, ff)], w_sem.at[min(i, 1)]),
            pltpu.make_async_copy(w_up.at[at, :], wgu.at[at, pl.ds(ff, ff)], w_sem.at[min(i, 1)]),
        ]

    def split_grads(b, d_hidden):
        slot, at = lax.rem(b, 2), rows_of(b)
        g, u = g_rows[slot].astype(F32), u_rows[slot].astype(F32)
        sig = jax.nn.sigmoid(g)
        silu = g * sig
        dgu[pl.ds(at, HALF), pl.ds(0, ff)] = (d_hidden * u * (sig + silu * (1.0 - sig))).astype(BF16)
        dgu[pl.ds(at, HALF), pl.ds(ff, ff)] = (d_hidden * silu).astype(BF16)
        hid[:, pl.ds(at, HALF)] = (silu * u).T.astype(BF16)

    def loaded(sem, blocks):
        at = pl.ds(0, blocks * block)
        pltpu.make_async_copy(wgu.at[at, :], wgu.at[at, :], w_sem.at[sem]).wait()

    @scoped
    def hidden_grads(b):
        for copy in row_copies(b):
            copy.wait()
        split_grads(b, dot(dy_rows[lax.rem(b, 2)], wd[...], NT))

        @pl.when(b + 2 < 2 * chunks)
        def _():
            for copy in row_copies(b + 2):
                copy.start()

    def first_copies(i):
        at = pl.ds(i * (width // PIECES), width // PIECES)
        return [
            pltpu.make_async_copy(dy.at[pl.ds(rows_of(0), HALF), at], dy_rows.at[0, :, at], first_sem.at[i, 0]),
            pltpu.make_async_copy(w_down.at[:, at], wd.at[:, at], first_sem.at[i, 1]),
        ]

    @scoped
    def first_grads():
        behind = [load_w(0), row_copies(1), load_w(1), load_w(2) + load_w(3)]
        d_hidden = None
        for i in range(PIECES):
            for copy in first_copies(i):
                copy.wait()
            for copy in behind[i]:
                copy.start()
            at = pl.ds(i * (width // PIECES), width // PIECES)
            part = dot(dy_rows[0, :, at], wd[:, at], NT)
            d_hidden = part if d_hidden is None else d_hidden + part
        for copy in row_copies(0, first=1):
            copy.wait()
        split_grads(0, d_hidden)
        for copy in row_copies(2):
            copy.start()

    def term(at, b):
        return dot(dgu[pl.ds(at, HALF), :], wgu[pl.ds(pl.multiple_of(b * block, 128), block), :], NT)

    @scoped
    def partner_block(k, o):
        @pl.when(jnp.logical_and(k == 0, o == 0))
        def _():
            loaded(0, 1)

        @pl.when(jnp.logical_and(k == 0, o == 1))
        def _():
            loaded(1, n - 1)

        pl.when(k > 0)(lambda: swap(k - 1, o).wait_send())
        outbox[o] = term(other(k), lax.rem(q1 + turn(o), n)).astype(BF16)
        swap(k, o).start()

    @scoped
    def own_block(k, o):
        pl.when(jnp.logical_and(k >= SLOTS, o == 0))(lambda: reduced(k - SLOTS))
        b = lax.rem(p1 + turn(o), n)
        t = term(own(k), b)
        swap_in(k, o).wait_recv()
        sums[lax.rem(k, SLOTS), b] = (t + mine[pl.ds(kept(k), HALF), pl.ds(cols(b), block)].astype(F32)).astype(BF16)
        pl.when(o == 0)(lambda: send(0, k, 0, 1))
        pl.when(o == 1)(lambda: send(0, k, 2))
        pl.when(o == 2)(lambda: send(0, k, 3))

    @scoped
    def weight_grads(u):
        for copy in col_copies(u):
            copy.wait()
        slot = lax.rem(u, 2)

        at = pl.ds(pl.multiple_of(u * COLS, COLS), COLS)
        wgu[at, :] = dot(x_cols[slot], dgu[...], TN).astype(BF16)
        wd[:, at] = dot(hid[...], dy_cols[slot], NN).astype(BF16)

        @pl.when(u + 2 < units)
        def _():
            for copy in col_copies(u + 2):
                copy.start()

    def add(dst, size, *srcs):
        step = 32

        @pl.loop(0, size // step)
        def _(r):
            at = pl.multiple_of(r * step, step)
            total = srcs[0](at, step).astype(F32)
            for s in srcs[1:]:
                total = total + s(at, step).astype(F32)
            dst(at, step, total.astype(BF16))

    def add_sums(k, b, off, size, lanes, *lands):
        def mine(at, step):
            return sums[lax.rem(k, SLOTS), b, pl.ds(off + at, step), lanes]

        def put(at, step, v):
            sums[lax.rem(k, SLOTS), b, pl.ds(off + at, step), lanes] = v

        add(put, size, mine, *lands)

    def landed(row, first, wide):
        return lambda at, step: theirs[pl.ds(row + at, step), pl.ds(first, wide)]

    @scoped
    def s1(k):
        @pl.when(k == chunks - 1)
        def _():
            for o in range(n):
                swap(k, o).wait_send()

        arrive(0, k, 0)
        add_sums(k, mod(p1 + n - 1), 0, hr, slice(None), landed(kept(k), 0, block))
        send(0, k, 4)
        arrive(0, k, 1)
        add_sums(k, mod(p1 + 1), hr, hr, slice(None), landed(kept(k) + hr, 0, block))
        send(0, k, 5)

    @scoped
    def s2(k):
        arrive_together(0, k, 2, theirs.at[pl.ds(kept(k), HALF), pl.ds(block, 2 * block)])
        add_sums(k, p1, 0, HALF, slice(None), landed(kept(k), block, block), landed(kept(k), 2 * block, block))
        send(1, k, 0, 1, 2, 3)

    @scoped
    def s3(k):
        base = 3 * block
        arrive(1, k, 0)
        add_sums(k, p1, pl.multiple_of(mod(p2 + n - 1) * sub, sub), sub, pl.ds(0, hc), landed(kept(k), base, hc))
        send(1, k, 4)
        arrive(1, k, 1)
        add_sums(k, p1, pl.multiple_of(mod(p2 + 1) * sub, sub), sub, pl.ds(hc, hc), landed(kept(k), base + hc, hc))
        send(1, k, 5)

    @scoped
    def s4(k):
        arrive_together(1, k, 2, theirs.at[pl.ds(kept(k) + sub, 2 * sub), pl.ds(3 * block, block)])
        off = pl.multiple_of(p2 * sub, sub)

        def put(at, step, v):
            mine[pl.ds(kept(k) + off + at, step), pl.ds(cols(p1), block)] = v

        add(
            put, sub,
            lambda at, step: sums[lax.rem(k, SLOTS), p1, pl.ds(off + at, step), :],
            landed(kept(k) + sub, 3 * block, block),
            landed(kept(k) + 2 * sub, 3 * block, block),
        )
        send(2, k, 0, 1, 2, 3)
        pl.when(k == chunks - 1)(lambda: send(3, k, 0, 1))
        pl.semaphore_signal(credit.at[k], inc=1, device_id={"tp": partner}, device_id_type=MESH)

    @scoped
    def s5(k):
        arrive(2, k, 0)
        send(2, k, 4)
        arrive(2, k, 1)
        send(2, k, 5)

    @scoped
    def s6(k):
        pl.when(k < chunks - 1)(lambda: send(3, k, 0, 1))
        arrive(2, k, 2)
        send(3, k, 2)
        arrive(2, k, 3)
        send(3, k, 4, 5)
        arrive_together(2, k, 4, mine.at[pl.ds(kept(k), sub), pl.ds(cols(p1), block)])
        send(3, k, 6, 7, 3)
        pl.semaphore_wait(credit.at[k], 1)
        share(k, 0).start()

    @scoped
    def s7(k):
        for came, on in ((0, 8), (5, 9), (2, 10), (7, 11)):
            arrive(3, k, came)
            send(3, k, on)

    @scoped
    def s8(k):
        pl.when(k >= chunks - SLOTS)(lambda: reduced(k))
        left_together(2, k, mine.at[pl.ds(kept(k), 3 * sub), pl.ds(0, block)])
        arrive_together(3, k, 4, mine.at[pl.ds(kept(k), hr), pl.ds(cols(mod(p1 + 1)), block)])
        share(k, 1).start()
        arrive_together(3, k, 1, mine.at[pl.ds(kept(k), hr), pl.ds(cols(mod(p1 + n - 1)), block)])
        share(k, 2).start()
        for came, i in ((8, 3), (9, 5), (10, 4), (11, 6)):
            arrive(3, k, came)
            share(k, i).start()

    @scoped
    def s9(k):
        whole = pl.ds(kept(k), HALF)
        together(theirs.at[whole, :], share_send.at[k], pair_recv.at[k, n]).wait_recv()
        left_together(3, k, sums.at[lax.rem(k, SLOTS), pl.ds(0, 3)])
        together(mine.at[whole, :], share_send.at[k], pair_recv.at[k, n]).wait_send()

    def matmuls(t):
        k, r = t // PERIOD, lax.rem(t, PERIOD)
        first = r < 4
        even = lax.rem(r, 2) == 0
        to_partner = jnp.logical_or(r == 1, jnp.logical_or(r == 3, jnp.logical_or(r == 5, r == 7)))
        to_own = jnp.logical_or(r == 4, jnp.logical_or(r == 6, r >= 8))
        grads = jnp.logical_and(first, even)
        pl.when(jnp.logical_and(grads, t > 0))(lambda: hidden_grads(2 * k + r // 2))
        pl.when(to_partner)(lambda: partner_block(k, r // 2))
        pl.when(to_own)(lambda: own_block(k, r // 6 + r // 8 + r // 9))

    stages = (s1, s2, s3, s4, s5, s6, s7, s8, s9)
    work = chunks * PERIOD

    barrier = pltpu.get_barrier_semaphore()
    for to in (left1, right1, left2, right2, partner):
        pl.semaphore_signal(barrier, inc=1, device_id={"tp": to}, device_id_type=MESH)
    for i in range(PIECES):
        for copy in first_copies(i):
            copy.start()
    for copy in row_copies(0, first=1):
        copy.start()
    first_grads()
    with jax.named_scope("meet"):
        pl.semaphore_wait(barrier, 5)

    @pl.loop(0, TICKS[-1][-1] + 1)
    def _(t):
        pl.when(t < work)(lambda: matmuls(t))

        @pl.when(t == PERIOD)
        def _():
            for u in range(2):
                for copy in col_copies(u):
                    copy.start()

        pl.when(jnp.logical_and(t >= work, t < work + units))(lambda: weight_grads(t - work))
        for stage, ticks in zip(stages, TICKS):
            now, k = t == ticks[0], 0
            for tick in ticks[1:]:
                now = jnp.logical_or(now, t == tick)
                k = k + (t >= tick).astype(jnp.int32)
            pl.when(now)(functools.partial(stage, k))


def store(dw_gu, dw_d, mine, theirs, dx, dw_gate, dw_up, dw_down, sem):
    c = lax.rem(lax.axis_index("tp"), 2)
    ff = dw_gate.shape[1]
    pairs = [(dw_gu.at[:, pl.ds(0, ff)], dw_gate), (dw_gu.at[:, pl.ds(ff, ff)], dw_up), (dw_d, dw_down)]
    for k in range(mine.shape[0] // HALF):
        for half, core in ((mine, c), (theirs, 1 - c)):
            at = pl.ds(pl.multiple_of((2 * k + core) * HALF, HALF), HALF)
            pairs.append((half.at[pl.ds(k * HALF, HALF), :], dx.at[at, :]))
    copies = [pltpu.make_async_copy(src, dst, sem.at[i]) for i, (src, dst) in enumerate(pairs)]
    for copy in copies:
        copy.start()
    for copy in copies:
        copy.wait()


def solution(mesh):
    n = math.isqrt(mesh.shape["tp"] // 2)
    if n != 4 or 2 * n * n != mesh.shape["tp"]:
        raise ValueError("unexpected group")

    def step(x, dy, gate, up, w_gate, w_up, w_down):
        rows, width = x.shape
        ff = gate.shape[1]
        chunks, block = rows // (2 * HALF), width // n
        any_space = pl.BlockSpec(memory_space=pl.ANY)
        vmem = pl.BlockSpec(memory_space=pltpu.VMEM)
        dma = pltpu.SemaphoreType.DMA
        kept = pl.pallas_call(
            functools.partial(kernel, n),
            out_shape=(
                pltpu.VMEM((width, 2 * ff), BF16),
                pltpu.VMEM((ff, width), BF16),
                pltpu.VMEM((rows // 2, width), BF16),
                pltpu.VMEM((rows // 2, width), BF16),
            ),
            in_specs=[any_space] * 7,
            out_specs=[vmem] * 4,
            scratch_shapes=[
                pltpu.VMEM((rows, 2 * ff), BF16),
                pltpu.VMEM((ff, rows), BF16),
                pltpu.VMEM((SLOTS, n, HALF, block), BF16),
                pltpu.VMEM((n, HALF, block), BF16),
                pltpu.VMEM((2, HALF, width), BF16),
                pltpu.VMEM((2, HALF, ff), BF16),
                pltpu.VMEM((2, HALF, ff), BF16),
                pltpu.VMEM((2, rows, COLS), BF16),
                pltpu.VMEM((2, rows, COLS), BF16),
                dma((chunks, 4)),
                dma((chunks, 21)),
                dma((n,)),
                dma((chunks,)),
                dma((chunks, n + 1)),
                pltpu.SemaphoreType.REGULAR((chunks,)),
                dma((2,)),
                dma((PIECES, 2)),
                dma((2, 3)),
                dma((2, 2)),
            ],
            compiler_params=pltpu.CompilerParams(
                collective_id=0, has_side_effects=True, vmem_limit_bytes=31 * 1024 * 1024
            ),
        )(x, dy, gate, up, w_gate, w_up, w_down)
        return pl.pallas_call(
            store,
            out_shape=[jax.ShapeDtypeStruct(a.shape, BF16) for a in (x, w_gate, w_up, w_down)],
            in_specs=[vmem] * 4,
            out_specs=[any_space] * 4,
            scratch_shapes=[dma((3 + rows // HALF,))],
            compiler_params=pltpu.CompilerParams(vmem_limit_bytes=1024 * 1024),
        )(*kept)

    tokens, columns, by_rows = P("dp", None), P(None, "tp"), P("tp", None)
    return jax.shard_map(
        step,
        mesh=mesh,
        in_specs=(tokens, tokens, P("dp", "tp"), P("dp", "tp"), columns, columns, by_rows),
        out_specs=(tokens, P("dp", "tp"), P("dp", "tp"), P(("dp", "tp"), None)),
        check_vma=False,
    )
```
